32 devices in a mesh: dom: 8 (over y, x, core), grp: 4 (over z).
Axes of the slice: x: 2, y: 2, z: 4, core: 2. Of those that a mesh axis runs over, the one named last changes fastest.
Arguments:
- features: bfloat16 [65536, 256], P(('dom', 'grp')), may hold values from -6 to 6
- edge_src: int32 [524288], P(('dom', 'grp')), may hold values from 0 to 2303, as said below
- edge_dst: int32 [524288], P(('dom', 'grp')), may hold values from 0 to 2047, as said below
- edge_count: int32 [32], P(('dom', 'grp')), may hold values from 4096 to 16384, as said below
- halo_index: int32 [32, 32, 8], P(('dom', 'grp')), may hold values from 0 to 2047
- request_rows: int32 [32, 32, 16], P(('dom', 'grp')), may hold values from 0 to 2047, as said below
- pair_ends: int32 [65536, 2], P(('dom', 'grp')), may hold values from 0 to 511
- labels: int32 [65536], P(('dom', 'grp')), may hold values 0 or 1
- pair_weight: float32 [65536], P(('dom', 'grp')), may hold values from 0.25 to 4
- w_self: bfloat16 [256, 256], replicated, may hold values from -0.375 to 0.375
- w_neigh: bfloat16 [256, 256], replicated, may hold values from -0.375 to 0.375
- w_hidden: bfloat16 [512, 256], replicated, may hold values from -0.25 to 0.25
- b_hidden: float32 [256], replicated, may hold values from -3 to 3
- w_out: float32 [256], replicated, may hold values from -0.375 to 0.375
Outputs:
- logits: float32 [65536], P(('dom', 'grp'))
- grad_features: float32 [65536, 256], P(('dom', 'grp'))
- grad_w_self: float32 [256, 256], replicated
- grad_w_neigh: float32 [256, 256], replicated
- grad_w_hidden: float32 [512, 256], replicated
- grad_b_hidden: float32 [256], replicated
- grad_w_out: float32 [256], replicated
The draws below stay inside these ranges and needn't reach their ends.
Inputs may be any that keep to these rules, and one draw needn't show every extreme that they name: `edge_src`: a row of the partition's own table. `edge_dst`: a local node of the partition; slots at or past edge_count are not live and hold arbitrary values. `edge_count`: some partition has exactly 16384 live slots. `halo_index`: local rows of the sending partition; 8 to every partition, itself included. `request_rows`: local rows of the owning partition, distinct and increasing within each list of 16. `pair_ends`: rows of the shard's own received rows.
All inputs are finite; a program needn't handle non-finite values. No bound on the sum of `labels` on one device may be relied on, other than what follows from the above.
Results may differ from the reference program's by a relative error of at most 0.02.
The reference program's roundings to bfloat16 on the way count: a program that leaves them out, or rounds other values in their place, can miss the bound.
Values may be sent and summed in bfloat16 or wider, within the bound.
A program may use at most 192 MiB of HBM per device.

```python
import math
import jax
import jax.numpy as jnp
from jax import lax

D = 256
NODE_DEV = 2048
HALO = 8
REQ = 16
TE_DEV = 2048
PARTITIONS = 32
EDGE_DEV = 16384
NODES = 65536
EDGES = 524288
TRAIN = 65536
RECEIVED = 512


def draw_edge_src(key, part):
    key_one, key_two, key_three = jax.random.split(key, 3)
    coin_flip = jax.random.randint(key_one, (EDGES,), 0, 2)
    local_rows = jax.random.randint(key_two, (EDGES,), 0, NODE_DEV)
    remote_rows = NODE_DEV + jax.random.randint(key_three, (EDGES,), 0, HALO * PARTITIONS)
    return jnp.where(coin_flip == 0, local_rows, remote_rows).astype(jnp.int32)


def draw_edge_dst(key, part):
    key_one, key_two = jax.random.split(key, 2)
    first_draw = jax.random.randint(key_one, (EDGES,), 0, NODE_DEV)
    second_draw = jax.random.randint(key_two, (EDGES,), 0, NODE_DEV)
    return (first_draw * second_draw // (NODE_DEV - 1)).astype(jnp.int32)


def draw_edge_count(key, part):
    key_one, key_two = jax.random.split(key, 2)
    divisor = 1 + jax.random.randint(key_one, (PARTITIONS,), 0, 4)
    counts = EDGE_DEV // divisor
    full_one = jax.random.randint(key_two, (), 0, PARTITIONS)
    return jnp.where(jnp.arange(PARTITIONS) == full_one, EDGE_DEV, counts).astype(jnp.int32)


def draw_request_rows(key, part):
    stride = NODE_DEV // REQ
    offsets = jax.random.randint(key, (PARTITIONS, PARTITIONS, REQ), 0, stride)
    return (jnp.arange(REQ, dtype=jnp.int32)[None, None, :] * stride + offsets).astype(jnp.int32)


def set_ends(entries, stream_key, smallest, top_value):
    shape = entries.shape
    spot = [jax.random.randint(jax.random.fold_in(stream_key, axis), (), 0, shape[axis]) for axis in range(len(shape))]
    entries = entries.at[tuple(spot)].set(smallest)
    longest = shape.index(max(shape))
    spot[longest] = (spot[longest] + 1) % shape[longest]
    return entries.at[tuple(spot)].set(top_value)


def levels(key, extent, cuts, smallest, top_value):
    level = 1.0
    for dim, shards_of in cuts:
        heights = jax.random.uniform(jax.random.fold_in(jax.random.fold_in(key, 6), dim), (shards_of,), jnp.float32, smallest / len(cuts), top_value / len(cuts))
        level = level * jnp.repeat(jnp.exp(heights), extent[dim] // shards_of).reshape((-1,) + (1,) * (len(extent) - 1 - dim))
    return level


def noise(own_key, extent, width, most, cuts=(), kind=jnp.bfloat16):
    level = levels(own_key, extent, cuts, -0.22, 0.18) if cuts else 1.0
    entries = jax.random.normal(own_key, extent, jnp.float32) * width * level
    return jnp.minimum(jnp.maximum(entries, -most), most).astype(kind)


def setup_inputs(seed: int = 0) -> dict:
    streams_of = jax.random.split(jax.random.key(seed), 15)
    features = noise(streams_of[0], (NODES, D), 1.0, 6.0, ((0, 32),))
    edge_src = draw_edge_src(jax.random.fold_in(streams_of[14], 71), 0)
    edge_dst = draw_edge_dst(jax.random.fold_in(streams_of[14], 71), 0)
    edge_count = draw_edge_count(jax.random.fold_in(streams_of[14], 71), 0)
    halo_index = set_ends(jax.random.randint(streams_of[4], (PARTITIONS, PARTITIONS, HALO), 0, NODE_DEV), jax.random.fold_in(streams_of[4], 1), 0, NODE_DEV - 1).astype(jnp.int32)
    request_rows = draw_request_rows(jax.random.fold_in(streams_of[14], 71), 0)
    pair_ends = set_ends(jax.random.randint(streams_of[6], (TRAIN, 2), 0, RECEIVED), jax.random.fold_in(streams_of[6], 1), 0, RECEIVED - 1).astype(jnp.int32)
    labels = set_ends((jax.random.randint(streams_of[7], (TRAIN,), 0, 2) < 1).astype(jnp.int32), jax.random.fold_in(streams_of[7], 1), 0, 1)
    pair_weight = jnp.clip(jnp.exp(math.log(4.0) - 2.7725887 * jax.random.uniform(streams_of[8], (TRAIN,), jnp.float32) ** levels(streams_of[8], (TRAIN,), ((0, 32),), -0.2, 0.2)), 0.25, 4.0)
    w_self = noise(streams_of[9], (D, D), D ** -0.5, 0.375)
    w_neigh = noise(streams_of[10], (D, D), D ** -0.5, 0.375)
    w_hidden = noise(streams_of[11], (2 * D, D), (2 * D) ** -0.5, 0.25)
    b_hidden = noise(streams_of[12], (D,), 0.5, 3.0, (), jnp.float32)
    w_out = noise(streams_of[13], (D,), D ** -0.5, 0.375, (), jnp.float32)
    return dict(features=features, edge_src=edge_src, edge_dst=edge_dst, edge_count=edge_count, halo_index=halo_index, request_rows=request_rows, pair_ends=pair_ends, labels=labels, pair_weight=pair_weight, w_self=w_self, w_neigh=w_neigh, w_hidden=w_hidden, b_hidden=b_hidden, w_out=w_out)


def encode_one(own_rows, halo_rows, src_slots, dst_slots, live_count, w_self, w_neigh):
    row_table = jnp.concatenate([own_rows, halo_rows], axis=0)
    slot_ids = jnp.arange(src_slots.shape[0], dtype=jnp.int32)
    alive_slot = slot_ids < live_count
    dst_index = jnp.where(alive_slot, dst_slots, NODE_DEV).astype(jnp.int32)
    gathered = row_table[src_slots].astype(jnp.float32)
    agg_sums = jax.ops.segment_sum(gathered, dst_index, num_segments=NODE_DEV + 1)[:NODE_DEV]
    degree = jax.ops.segment_sum(alive_slot.astype(jnp.float32), dst_index, num_segments=NODE_DEV + 1)[:NODE_DEV]
    aggregate = (agg_sums / jnp.maximum(degree, 1.0)[:, None]).astype(jnp.bfloat16)
    embedding = (jnp.dot(own_rows, w_self, preferred_element_type=jnp.float32)
                 + jnp.dot(aggregate, w_neigh, preferred_element_type=jnp.float32)).astype(jnp.bfloat16)
    return embedding, aggregate, degree


def reference(features, edge_src, edge_dst, edge_count, halo_index, request_rows, pair_ends, labels, pair_weight, w_self, w_neigh, w_hidden, b_hidden, w_out):
    part_count = PARTITIONS
    own_rows = features.reshape(part_count, NODE_DEV, D)
    senders = jnp.arange(part_count, dtype=jnp.int32)[:, None, None]
    sent_rows = own_rows[senders, halo_index]
    arriving = jnp.transpose(sent_rows, (1, 0, 2, 3)).reshape(part_count, part_count * HALO, D)
    src_slots = edge_src.reshape(part_count, EDGE_DEV)
    dst_slots = edge_dst.reshape(part_count, EDGE_DEV)

    def encode_step(packed):
        return encode_one(packed[0], packed[1], packed[2], packed[3], packed[4], w_self, w_neigh)

    embedding, aggregate, degree = lax.map(encode_step, (own_rows, arriving, src_slots, dst_slots, edge_count))

    end_pairs = pair_ends.reshape(part_count, TE_DEV, 2)
    flag_rows = labels.reshape(part_count, TE_DEV).astype(jnp.float32)
    weight_rows = pair_weight.reshape(part_count, TE_DEV)
    owners = jnp.arange(part_count, dtype=jnp.int32)[:, None]

    def decode_step(carry, packed):
        emb_grad, grad_hidden, grad_bias, grad_out = carry
        wanted_rows, pair_end, flag_row, weight_row = packed
        received = embedding[owners, wanted_rows].reshape(part_count * REQ, D)
        pair_input = jnp.concatenate([received[pair_end[:, 0]], received[pair_end[:, 1]]], axis=1)
        pre_act = jnp.dot(pair_input, w_hidden, preferred_element_type=jnp.float32) + b_hidden
        hidden = jnp.maximum(pre_act, 0.0)
        logits = jnp.dot(hidden, w_out, precision=lax.Precision.HIGHEST)
        slope_term = weight_row * (jax.nn.sigmoid(logits) - flag_row)
        grad_out = grad_out + jnp.dot(slope_term, hidden, precision=lax.Precision.HIGHEST)
        delta_act = jnp.where(pre_act > 0, slope_term[:, None] * w_out[None, :], 0.0)
        grad_bias = grad_bias + jnp.sum(delta_act, axis=0)
        delta_b = delta_act.astype(jnp.bfloat16)
        grad_hidden = grad_hidden + jnp.dot(pair_input.T, delta_b, preferred_element_type=jnp.float32)
        pair_grad = jnp.dot(delta_b, w_hidden.T, preferred_element_type=jnp.float32)
        received_grad = (jax.ops.segment_sum(pair_grad[:, :D], pair_end[:, 0], num_segments=part_count * REQ)
                         + jax.ops.segment_sum(pair_grad[:, D:], pair_end[:, 1], num_segments=part_count * REQ))
        received_grad_b = lax.optimization_barrier(received_grad.astype(jnp.bfloat16))
        emb_grad = emb_grad.at[owners, wanted_rows].add(received_grad_b.astype(jnp.float32).reshape(part_count, REQ, D))
        return (emb_grad, grad_hidden, grad_bias, grad_out), logits

    start = (jnp.zeros((part_count, NODE_DEV, D), jnp.float32), jnp.zeros((2 * D, D), jnp.float32),
             jnp.zeros((D,), jnp.float32), jnp.zeros((D,), jnp.float32))
    final, logit_rows = lax.scan(decode_step, start, (request_rows, end_pairs, flag_rows, weight_rows))
    emb_grad, grad_hidden, grad_bias, grad_out = final
    grad_b = emb_grad.astype(jnp.bfloat16)

    def encode_back(packed):
        own_part, agg_part, deg_part, grad_part, src_part, dst_part, count_part = packed
        grad_self = jnp.dot(own_part.T, grad_part, preferred_element_type=jnp.float32)
        grad_neigh = jnp.dot(agg_part.T, grad_part, preferred_element_type=jnp.float32)
        direct = jnp.dot(grad_part, w_self.T, preferred_element_type=jnp.float32)
        agg_grad = jnp.dot(grad_part, w_neigh.T, preferred_element_type=jnp.float32) / jnp.maximum(deg_part, 1.0)[:, None]
        padded = jnp.concatenate([agg_grad, jnp.zeros((1, D), jnp.float32)], axis=0)
        slot_ids = jnp.arange(src_part.shape[0], dtype=jnp.int32)
        dst_index = jnp.where(slot_ids < count_part, dst_part, NODE_DEV).astype(jnp.int32)
        table_grad = jax.ops.segment_sum(padded[dst_index], src_part, num_segments=NODE_DEV + part_count * HALO)
        return (direct + table_grad[:NODE_DEV], table_grad[NODE_DEV:].reshape(part_count, HALO, D), grad_self, grad_neigh)

    local_grad, halo_back, self_terms, neigh_terms = lax.map(
        encode_back, (own_rows, aggregate, degree, grad_b, src_slots, dst_slots, edge_count))
    returned = jnp.transpose(halo_back, (1, 0, 2, 3))
    local_grad = local_grad.at[senders, halo_index].add(returned)
    return (logit_rows.reshape(part_count * TE_DEV), local_grad.reshape(part_count * NODE_DEV, D),
            jnp.sum(self_terms, axis=0), jnp.sum(neigh_terms, axis=0), grad_hidden, grad_bias, grad_out)
```

```python
import functools

import jax
import jax.numpy as jnp
from jax import lax
from jax.experimental import pallas as pl
from jax.experimental.pallas import tpu as pltpu
from jax.sharding import PartitionSpec as P

F32 = jnp.float32
BF16 = jnp.bfloat16
F8 = jnp.float8_e4m3fn
VMEM_LIMIT = 60 * 1024 * 1024
NN = (((1,), (0,)), ((), ()))
NT = (((1,), (1,)), ((), ()))
TN = (((0,), (0,)), ((), ()))


def dot(left, right, dims=NN):
    return lax.dot_general(left, right, dims, preferred_element_type=F32)


def column_of(row):
    return jnp.broadcast_to(row, (128, row.shape[1])).T[:, :1]


def row_of(column):
    return jnp.broadcast_to(column, (column.shape[0], 128)).T[:1, :]


def equal_mask(left, right):
    return jnp.where(left == right, 1.0, 0.0).astype(BF16)


def iota(shape, dim):
    return lax.broadcasted_iota(jnp.int32, shape, dim).astype(F32)


class Links:
    def __init__(self, peers, grp):
        self.peers, self.grp = peers, grp
        self.me = lax.axis_index("dom") * grp + lax.axis_index("grp")

    def device(self, peer):
        return {"dom": peer // self.grp, "grp": lax.rem(peer, self.grp)}

    def other(self, step):
        return lax.rem(self.me + step, self.peers)

    def each(self, body):
        def step(i, carry):
            body(self.other(i))
            return carry

        lax.fori_loop(1, self.peers, step, 0)

    def greet(self):
        barrier = pltpu.get_barrier_semaphore()
        self.each(lambda peer: pl.semaphore_signal(
            barrier, inc=1, device_id=self.device(peer), device_id_type=pl.DeviceIdType.MESH))

    def greeted(self):
        pl.semaphore_wait(pltpu.get_barrier_semaphore(), self.peers - 1)

    def copy(self, src, dst, send, recv, peer, slot):
        return pltpu.make_async_remote_copy(
            src_ref=src, dst_ref=dst, send_sem=send.at[peer], recv_sem=recv.at[slot],
            device_id=self.device(peer), device_id_type=pl.DeviceIdType.MESH)

    def start(self, moves):
        def one(peer):
            for pick, dst, send, recv in moves:
                self.copy(pick(peer), dst.at[self.me], send, recv, peer, self.me).start()

        self.each(one)

    def finish(self, moves):
        def one(peer):
            for pick, dst, send, recv in moves:
                copy = self.copy(pick(peer), dst.at[peer], send, recv, peer, peer)
                copy.wait_recv()
                copy.wait_send()

        self.each(one)


def block_of(ref):
    return lambda peer: ref.at[peer]


def whole_of(ref):
    return lambda peer: ref


def sems(peers, count):
    return [pltpu.SemaphoreType.DMA((peers,)) for _ in range(2 * count)]


def call(body, outs, args, scratch=(), collective_id=None, smem=(), limit=VMEM_LIMIT):
    params = dict(vmem_limit_bytes=limit)
    if collective_id is not None:
        params.update(collective_id=collective_id, has_side_effects=True)
    return pl.pallas_call(
        body,
        out_shape=tuple(jax.ShapeDtypeStruct(s, d) for s, d in outs),
        in_specs=[
            pl.BlockSpec(memory_space=pltpu.SMEM if i in smem else pltpu.VMEM)
            for i in range(len(args))
        ],
        out_specs=tuple(pl.BlockSpec(memory_space=pltpu.VMEM) for _ in outs),
        scratch_shapes=list(scratch),
        compiler_params=pltpu.CompilerParams(**params),
    )(*args)


def spread_column(rows, length):
    peers = rows.shape[0]
    spread = jnp.broadcast_to(rows, (peers, length, 128)).reshape(peers * length, 128)
    lane = lax.broadcasted_iota(jnp.int32, spread.shape, 1)
    row = lax.rem(lax.broadcasted_iota(jnp.int32, spread.shape, 0), length)
    return jnp.sum(jnp.where(lane == row, spread, 0.0), axis=1, keepdims=True)


def halo_column(halo, turned):
    halo_len, peers = halo.shape
    turned[...] = jnp.zeros_like(turned)
    turned[:halo_len, :peers] = halo[...].astype(F32)
    return spread_column(turned[...].T[:peers].reshape(peers, 1, 128), halo_len)


def first_exchange(peers, grp, feat, halo, request, wanted, arrived, turned, asked, outgoing, s0, r0, s1, r1):
    links = Links(peers, grp)
    me = links.me
    links.greet()
    nodes = feat.shape[0]
    turned[...] = jnp.zeros_like(turned)
    turned[: request.shape[0], :peers] = request[...].astype(F32)
    asked[...] = turned[...].T[:peers].astype(jnp.int32).reshape(asked.shape)
    index = halo_column(halo, turned)
    pick = equal_mask(index, iota((index.shape[0], nodes), 1))
    outgoing[...] = dot(pick, feat[...]).astype(BF16).reshape(outgoing.shape)
    links.greeted()
    moves = [(block_of(asked), wanted, s0, r0), (block_of(outgoing), arrived, s1, r1)]
    links.start(moves)
    wanted[me] = asked[me]
    arrived[me] = outgoing[me]
    links.finish(moves)


def count_edges(req_len, nodes, block, group, src, dst, count, wanted, counts, total, marks, index, ranks, packs, dense):
    rows, table_rows = counts.shape
    depth = src.shape[0]
    bits = nodes.bit_length() - 1
    total[...] = jnp.zeros_like(total)
    column = spread_column(wanted[...].astype(F32), req_len)
    index[...] = jnp.broadcast_to(column, index.shape)
    high = jnp.floor(column * (1.0 / 128.0))
    low = column - high * 128.0
    lanes = iota((rows, 128), 1)
    seen = dot(equal_mask(high, lanes), equal_mask(low, lanes), TN)[: nodes // 128]
    power = lax.shift_left(jnp.ones(seen.shape, jnp.int32), lax.broadcasted_iota(jnp.int32, seen.shape, 0))
    word = jnp.sum(jnp.where(seen > 0.5, power, 0), axis=0, keepdims=True)
    slot = lax.broadcasted_iota(jnp.int32, src.shape, 0) * 128 + lax.broadcasted_iota(jnp.int32, src.shape, 1)
    live = slot < count[0]
    into = jnp.where(live, dst[...], 0)
    flags = jnp.take_along_axis(
        jnp.broadcast_to(word, src.shape), lax.bitwise_and(into, 127), axis=1, mode="promise_in_bounds")
    flag = lax.bitwise_and(lax.shift_right_logical(flags, lax.shift_right_logical(into, 7)), 1)
    active = jnp.where(live, flag, 0)
    ahead = jnp.where(iota((depth, depth), 1) < iota((depth, depth), 0), 1.0, 0.0).astype(BF16)
    amount = active.astype(F32)
    rank = dot(ahead, amount.astype(BF16))
    ranks[...] = jnp.where(active > 0, rank, -1.0)
    packs[...] = src[...] * nodes + into
    longest = jnp.max(jnp.sum(amount, axis=0, keepdims=True)).astype(jnp.int32)
    spots = iota((8, 128), 0)
    held = [jnp.full((8, 128), -1, jnp.int32) for _ in range(depth // 8)]
    for r in range(depth):
        to = jnp.broadcast_to(ranks[r : r + 1, :], (8, 128))
        value = jnp.broadcast_to(packs[r : r + 1, :], (8, 128))
        for b in range(r // 8 + 1):
            held[b] = jnp.where(to == spots + 8.0 * b, value, held[b])
    for b in range(depth // 8):
        dense[8 * b : 8 * b + 8, :] = held[b]

    ladder = iota((block, 128), 0).astype(BF16)

    @pl.loop(0, (longest + group - 1) // group)
    def _(c):
        highs, lows = [], []
        for k in range(group):
            value = dense[pl.ds(c * group + k, 1), :]
            node = jnp.where(value < 0, -1, lax.bitwise_and(value, nodes - 1)).astype(F32)
            marks[:, k * 128 : k * 128 + 128] = jnp.where(index[...] == node, 1.0, 0.0).astype(F8)
            source = lax.shift_right_arithmetic(value, bits)
            highs.append(lax.shift_right_arithmetic(source, block.bit_length() - 1))
            lows.append(lax.bitwise_and(source, block - 1))

        @pl.loop(0, table_rows // block)
        def _(b):
            hits = []
            for k in range(group):
                here = jnp.where(highs[k] == b, lows[k], -1).astype(F32).astype(BF16)
                hits.append(jnp.where(ladder == here, jnp.array(1, BF16), jnp.array(0, BF16)).astype(F8))
            cols = pl.ds(pl.multiple_of(b * block, block), block)
            total[:, cols] += dot(marks[...], jnp.concatenate(hits, axis=1), NT)

    counts[...] = total[...].astype(BF16)


def middle(
    peers, grp, req_len, chunk, block,
    feat, arrived, counts, wanted, halo, w_self, w_neigh, w_hidden, bias, w_out, ends, labels, weight,
    logits, out, g_s, g_n, g_h, g_b, g_o,
    turned, index, feat_w, agg_w, floor, served, received, picks, upper_lower, sums,
    back_sent, back, hidden_sent, hidden_in, hidden_own, hidden_all,
    small, small_in, grad, node_sent, node_in, node_own, node_all, near, far, returned, halo_back,
    s0, r0, s1, r1, s2, r2, s3, r3, s4, r4, s5, r5, s6, r6, s7, r7,
):
    links = Links(peers, grp)
    me = links.me
    nodes, width = feat.shape
    rows, table_rows = counts.shape
    size, parts = row_blocks(rows)
    links.greet()
    index[...] = jnp.broadcast_to(spread_column(wanted[...].astype(F32), req_len), index.shape)
    per = size // req_len
    for i in range(parts):
        span = slice(i * size, i * size + size)
        degree = jnp.sum(counts[span, :].astype(F32), axis=1, keepdims=True)
        floor_deg = jnp.maximum(degree, 1.0)
        total = dot(counts[span, :nodes], feat[...])
        total += dot(counts[span, nodes:], arrived[...].reshape(table_rows - nodes, width))
        agg = (total / floor_deg).astype(BF16)
        own = dot(equal_mask(index[span, :1], iota((size, nodes), 1)), feat[...]).astype(BF16)
        emb = (dot(own, w_self[...]) + dot(agg, w_neigh[...])).astype(BF16)
        served[i * per : i * per + per] = emb.reshape(per, req_len, width)
        feat_w[span, :] = own
        agg_w[span, :] = agg
        floor[span, :] = jnp.broadcast_to(floor_deg, (size, 128))
    links.greeted()
    serve = [(block_of(served), received, s0, r0)]
    links.start(serve)
    received[me] = served[me]
    pairs = ends.shape[1]
    slots = iota((rows, chunk), 0)

    @pl.loop(0, pairs // chunk)
    def _(c):
        span = pl.ds(pl.multiple_of(c * chunk, chunk), chunk)
        end = ends[:, span].astype(F32)
        picks[:rows, span] = equal_mask(slots, end[:1, :])
        picks[rows:, span] = equal_mask(slots, end[1:, :])

    bias_col = column_of(bias[...])
    out_col = column_of(w_out[...])
    sums[...] = jnp.zeros_like(sums)
    links.finish(serve)

    got = received[...].reshape(rows, width)
    for place, half in ((0, w_hidden[:width, :]), (rows, w_hidden[width:, :])):
        exact = dot(got, half).T
        upper = exact.astype(BF16)
        upper_lower[:width, place : place + rows] = upper
        upper_lower[width:, place : place + rows] = (exact - upper.astype(F32)).astype(BF16)

    def step(c, carry):
        bias_sum, out_sum = carry
        span = pl.ds(pl.multiple_of(c * chunk, chunk), chunk)
        both = dot(upper_lower[...], picks[:, span])
        pre = both[:width] + both[width:] + bias_col
        hidden = jnp.maximum(pre, 0.0)
        logit = jnp.sum(hidden * out_col, axis=0, keepdims=True)
        logits[:, span] = logit
        slope = weight[:, span] * (jax.nn.sigmoid(logit) - labels[:, span].astype(F32))
        delta = jnp.where(pre > 0, slope * out_col, 0.0)
        sums[...] += dot(picks[:, span], delta.astype(BF16), NT)
        return (
            bias_sum + jnp.sum(delta, axis=1, keepdims=True),
            out_sum + jnp.sum(hidden * slope, axis=1, keepdims=True),
        )

    zero = jnp.zeros((width, 1), F32)
    bias_sum, out_sum = lax.fori_loop(0, pairs // chunk, step, (zero, zero))
    left = sums[:rows, :].astype(BF16)
    right = sums[rows:, :].astype(BF16)
    back_rows = dot(left, w_hidden[:width, :], NT) + dot(right, w_hidden[width:, :], NT)
    back_sent[...] = back_rows.astype(BF16).reshape(back_sent.shape)
    give = [(block_of(back_sent), back, s1, r1)]
    links.start(give)
    back[me] = back_sent[me]

    small[0:1, :] = row_of(bias_sum)
    small[1:2, :] = row_of(out_sum)
    half = peers // 2
    shape = (half,) + hidden_sent.shape[1:]
    hidden_sent[:half] = dot(got, left, TN).astype(BF16).reshape(shape)
    hidden_sent[half:] = dot(got, right, TN).astype(BF16).reshape(shape)
    hidden_terms = [(block_of(hidden_sent), hidden_in, s2, r2), (whole_of(small), small_in, s3, r3)]
    links.start(hidden_terms)
    hidden_in[me] = hidden_sent[me]
    small_in[me] = small[...]
    other = row_of(index[:, :1])
    links.finish(give)

    for i in range(parts):
        span = slice(i * size, i * size + size)
        same = index[span, :1] == other
        first = lax.broadcasted_iota(jnp.int32, same.shape, 0) + i * size
        earlier = lax.broadcasted_iota(jnp.int32, same.shape, 1) < first
        repeat = jnp.sum(jnp.where(same & earlier, 1.0, 0.0), axis=1, keepdims=True)
        total = dot(jnp.where(same, 1.0, 0.0).astype(BF16), back[...].reshape(rows, width))
        grad[span, :] = jnp.where(repeat > 0.0, 0.0, total).astype(BF16)
    node_sent[:half] = dot(feat_w[...], grad[...], TN).astype(BF16).reshape(shape)
    node_sent[half:] = dot(agg_w[...], grad[...], TN).astype(BF16).reshape(shape)
    node_terms = [(block_of(node_sent), node_in, s4, r4)]
    links.start(node_terms)
    node_in[me] = node_sent[me]

    far[...] = (dot(grad[...], w_neigh[...], NT) / floor[:, :1]).astype(BF16)
    returned[...] = dot(counts[:, nodes:], far[...], TN).astype(BF16).reshape(returned.shape)
    send_back = [(block_of(returned), halo_back, s5, r5)]
    links.start(send_back)
    halo_back[me] = returned[me]

    near[...] = dot(grad[...], w_self[...], NT).astype(BF16)
    links.finish(hidden_terms)
    hidden_own[...] = jnp.sum(hidden_in[...].astype(F32), axis=0).astype(BF16)
    hidden_sums = [(whole_of(hidden_own), hidden_all, s6, r6)]
    links.start(hidden_sums)
    hidden_all[me] = hidden_own[...]

    def local(b, carry):
        cols = pl.ds(pl.multiple_of(b * block, block), block)
        spot = lax.broadcasted_iota(jnp.int32, (1, block), 1) + b * block
        pick = equal_mask(index[:, :1], spot.astype(F32))
        out[cols, :] = dot(counts[:, cols], far[...], TN) + dot(pick, near[...], TN)
        return carry

    lax.fori_loop(0, nodes // block, local, 0)
    links.finish(node_terms)
    node_own[...] = jnp.sum(node_in[...].astype(F32), axis=0).astype(BF16)
    node_sums = [(whole_of(node_own), node_all, s7, r7)]
    links.start(node_sums)
    node_all[me] = node_own[...]

    halo_row = row_of(halo_column(halo, turned))
    links.finish(send_back)

    def add(b, carry):
        cols = pl.ds(pl.multiple_of(b * block, block), block)
        spot = iota((block, halo_row.shape[1]), 0) + (b * block).astype(F32)
        out[cols, :] += dot(equal_mask(spot, halo_row), halo_back[...].reshape(halo_row.shape[1], width))
        return carry

    lax.fori_loop(0, nodes // block, add, 0)
    total = jnp.sum(small_in[...], axis=0)
    g_b[...] = total[0:1, :]
    g_o[...] = total[1:2, :]
    links.finish(hidden_sums)
    g_h[...] = hidden_all[...].astype(F32).reshape(g_h.shape)
    links.finish(node_sums)
    g_s[...] = node_all[:half].astype(F32).reshape(g_s.shape)
    g_n[...] = node_all[half:].astype(F32).reshape(g_n.shape)


def row_blocks(rows):
    size = min(rows, 512)
    return size, rows // size


def per_device(
    features, edge_src, edge_dst, edge_count, halo_index, request_rows, pair_ends,
    labels, pair_weight, w_self, w_neigh, w_hidden, b_hidden, w_out,
):
    nodes, width = features.shape
    grp = lax.axis_size("grp")
    peers = lax.axis_size("dom") * grp
    halo_len = halo_index.shape[2]
    req_len = request_rows.shape[2]
    slots = edge_src.shape[0]
    pairs = labels.shape[0]
    table_rows = nodes + peers * halo_len
    rows = peers * req_len
    block = 256
    part = 2 * width // peers
    turn = max(128, peers)

    halo = halo_index[0].T
    wanted, arrived = call(
        functools.partial(first_exchange, peers, grp),
        [((peers, 1, 128), jnp.int32), ((peers, halo_len, width), BF16)],
        (features, halo, request_rows[0].T),
        [
            pltpu.VMEM((128, turn), F32),
            pltpu.VMEM((peers, 1, 128), jnp.int32),
            pltpu.VMEM((peers, halo_len, width), BF16),
        ] + sems(peers, 2),
        collective_id=0,
    )
    group = 8
    depth = slots // 128
    (counts,) = call(
        functools.partial(count_edges, req_len, nodes, block, group),
        [((rows, table_rows), BF16)],
        (edge_src.reshape(depth, 128), edge_dst.reshape(depth, 128), edge_count, wanted),
        [
            pltpu.VMEM((rows, table_rows), F32),
            pltpu.VMEM((rows, group * 128), F8),
            pltpu.VMEM((rows, 128), F32),
            pltpu.VMEM((depth, 128), F32),
            pltpu.VMEM((depth, 128), jnp.int32),
            pltpu.VMEM((depth, 128), jnp.int32),
        ],
        smem=(2,),
    )
    chunk = 512
    rows_of = lambda *shape: pltpu.VMEM(shape, BF16)
    logits, grad_features, g_s, g_n, g_h, g_b, g_o = call(
        functools.partial(middle, peers, grp, req_len, chunk, block),
        [
            ((1, pairs), F32),
            ((nodes, width), F32),
            ((width, width), F32),
            ((width, width), F32),
            ((2 * width, width), F32),
            ((1, width), F32),
            ((1, width), F32),
        ],
        (
            features, arrived, counts, wanted, halo, w_self, w_neigh, w_hidden,
            b_hidden.reshape(1, width), w_out.reshape(1, width),
            pair_ends.T, labels.reshape(1, pairs), pair_weight.reshape(1, pairs),
        ),
        [
            pltpu.VMEM((128, turn), F32),
            pltpu.VMEM((rows, 128), F32),
            rows_of(rows, width),
            rows_of(rows, width),
            pltpu.VMEM((rows, 128), F32),
            rows_of(peers, req_len, width),
            rows_of(peers, req_len, width),
            rows_of(2 * rows, pairs),
            rows_of(2 * width, 2 * rows),
            pltpu.VMEM((2 * rows, width), F32),
            rows_of(peers, req_len, width),
            rows_of(peers, req_len, width),
            rows_of(peers, part, width),
            rows_of(peers, part, width),
            rows_of(part, width),
            rows_of(peers, part, width),
            pltpu.VMEM((2, width), F32),
            pltpu.VMEM((peers, 2, width), F32),
            rows_of(rows, width),
            rows_of(peers, part, width),
            rows_of(peers, part, width),
            rows_of(part, width),
            rows_of(peers, part, width),
            rows_of(rows, width),
            rows_of(rows, width),
            rows_of(peers, halo_len, width),
            rows_of(peers, halo_len, width),
        ] + sems(peers, 8),
        collective_id=1,
    )
    return (logits.reshape(pairs), grad_features, g_s, g_n, g_h, g_b.reshape(width), g_o.reshape(width))


def solution(mesh):
    both = ("dom", "grp")
    in_specs = (
        P(both, None), P(both), P(both), P(both), P(both, None, None), P(both, None, None),
        P(both, None), P(both), P(both), P(), P(), P(), P(), P(),
    )
    out_specs = (P(both), P(both, None), P(), P(), P(), P(), P())
    return jax.shard_map(
        per_device, mesh=mesh, in_specs=in_specs, out_specs=out_specs, check_vma=False
    )
```

```python
import functools

import jax
import jax.numpy as jnp
from jax import lax
from jax.experimental import pallas as pl
from jax.experimental.pallas import tpu as pltpu
from jax.sharding import PartitionSpec as P

F32 = jnp.float32
BF16 = jnp.bfloat16
F8 = jnp.float8_e4m3fn
VMEM_LIMIT = 60 * 1024 * 1024
K1LIM = 64 * 1024 * 1024 - 512 * 1024
GROUP = 8
NN = (((1,), (0,)), ((), ()))
NT = (((1,), (1,)), ((), ()))
TN = (((0,), (0,)), ((), ()))


def dot(left, right, dims=NN):
    return lax.dot_general(left, right, dims, preferred_element_type=F32)


def column_of(row):
    return jnp.broadcast_to(row, (128, row.shape[1])).T[:, :1]


def row_of(column):
    return jnp.broadcast_to(column, (column.shape[0], 128)).T[:1, :]


def equal_mask(left, right):
    return jnp.where(left == right, 1.0, 0.0).astype(BF16)


def iota(shape, dim):
    return lax.broadcasted_iota(jnp.int32, shape, dim).astype(F32)


class Links:
    def __init__(self, peers, grp):
        self.peers, self.grp = peers, grp
        self.me = lax.axis_index("dom") * grp + lax.axis_index("grp")

    def device(self, peer):
        return {"dom": peer // self.grp, "grp": lax.rem(peer, self.grp)}

    def other(self, step):
        return lax.rem(self.me + step, self.peers)

    def each(self, body):
        def step(i, carry):
            body(self.other(i))
            return carry

        lax.fori_loop(1, self.peers, step, 0)

    def greet(self):
        barrier = pltpu.get_barrier_semaphore()
        self.each(lambda peer: pl.semaphore_signal(
            barrier, inc=1, device_id=self.device(peer), device_id_type=pl.DeviceIdType.MESH))

    def greeted(self):
        pl.semaphore_wait(pltpu.get_barrier_semaphore(), self.peers - 1)

    def copy(self, src, dst, send, recv, peer, slot):
        return pltpu.make_async_remote_copy(
            src_ref=src, dst_ref=dst, send_sem=send.at[peer], recv_sem=recv.at[slot],
            device_id=self.device(peer), device_id_type=pl.DeviceIdType.MESH)

    def start(self, moves):
        def one(peer):
            for pick, dst, send, recv in moves:
                self.copy(pick(peer), dst.at[self.me], send, recv, peer, self.me).start()

        self.each(one)

    def finish(self, moves):
        def one(peer):
            for pick, dst, send, recv in moves:
                copy = self.copy(pick(peer), dst.at[peer], send, recv, peer, peer)
                copy.wait_recv()
                copy.wait_send()

        self.each(one)


class Line(Links):
    def __init__(self, axis, peers):
        self.axis, self.peers = axis, peers
        self.me = lax.axis_index(axis)

    def device(self, peer):
        return {self.axis: peer}


def block_of(ref):
    return lambda peer: ref.at[peer]


def whole_of(ref):
    return lambda peer: ref


def sems(peers, count):
    return [pltpu.SemaphoreType.DMA((peers,)) for _ in range(2 * count)]


def call(body, outs, args, scratch=(), collective_id=None, hbm=(), limit=VMEM_LIMIT, micros=0):
    params = dict(vmem_limit_bytes=limit)
    if collective_id is not None:
        params.update(collective_id=collective_id, has_side_effects=True)
    return pl.pallas_call(
        body,
        out_shape=tuple(jax.ShapeDtypeStruct(s, d) for s, d in outs),
        in_specs=[
            pl.BlockSpec(memory_space=pltpu.HBM if i in hbm else pltpu.VMEM)
            for i in range(len(args))
        ],
        out_specs=tuple(pl.BlockSpec(memory_space=pltpu.VMEM) for _ in outs),
        scratch_shapes=list(scratch),
        compiler_params=pltpu.CompilerParams(**params),
        cost_estimate=pl.CostEstimate(flops=micros * 10**9, bytes_accessed=1024, transcendentals=0) if micros else None,
    )(*args)


def spread_column(rows, length):
    peers = rows.shape[0]
    spread = jnp.broadcast_to(rows, (peers, length, 128)).reshape(peers * length, 128)
    lane = lax.broadcasted_iota(jnp.int32, spread.shape, 1)
    row = lax.rem(lax.broadcasted_iota(jnp.int32, spread.shape, 0), length)
    return jnp.sum(jnp.where(lane == row, spread, 0.0), axis=1, keepdims=True)


def halo_column(halo, turned):
    halo_len, peers = halo.shape
    turned[...] = jnp.zeros_like(turned)
    turned[:halo_len, :peers] = halo[...].astype(F32)
    return spread_column(turned[...].T[:peers].reshape(peers, 1, 128), halo_len)


def fetch(pairs, done):
    return [pltpu.make_async_copy(src, dst, done.at[i]) for i, (src, dst) in enumerate(pairs)]


def first_exchange(
    peers, grp, feat_far, halo_far, request_far, wanted, arrived,
    feat, halo, request, done, turned, asked, outgoing, s0, r0, s1, r1,
):
    links = Links(peers, grp)
    me = links.me
    loads = fetch([(request_far, request), (halo_far, halo), (feat_far, feat)], done)
    for load in loads:
        load.start()
    links.greet()
    nodes = feat.shape[0]
    loads[0].wait()
    loads[1].wait()
    turned[...] = jnp.zeros_like(turned)
    turned[: request.shape[0], :peers] = request[...].astype(F32)
    asked[...] = turned[...].T[:peers].astype(jnp.int32).reshape(asked.shape)
    index = halo_column(halo, turned)
    pick = equal_mask(index, iota((index.shape[0], nodes), 1))
    loads[2].wait()
    outgoing[...] = dot(pick, feat[...]).astype(BF16).reshape(outgoing.shape)
    links.greeted()
    moves = [(block_of(asked), wanted, s0, r0), (block_of(outgoing), arrived, s1, r1)]
    links.start(moves)
    wanted[me] = asked[me]
    arrived[me] = outgoing[me]
    links.finish(moves)


def count_edges(req_len, nodes, block, group, unroll, src_far, dst_far, count_far, wanted, counts, src, dst, count, done, total, marks, index, ranks, packs, dense):
    loads = fetch([(dst_far, dst), (src_far, src), (count_far, count)], done)
    for load in loads:
        load.start()
    rows, table_rows = counts.shape
    depth = src.shape[0]
    bits = nodes.bit_length() - 1
    total[...] = jnp.zeros_like(total)
    column = spread_column(wanted[...].astype(F32), req_len)
    index[...] = jnp.broadcast_to(column, index.shape)
    high = jnp.floor(column * (1.0 / 128.0))
    low = column - high * 128.0
    lanes = iota((rows, 128), 1)
    seen = dot(equal_mask(high, lanes), equal_mask(low, lanes), TN)[: nodes // 128]
    power = lax.shift_left(jnp.ones(seen.shape, jnp.int32), lax.broadcasted_iota(jnp.int32, seen.shape, 0))
    word = jnp.sum(jnp.where(seen > 0.5, power, 0), axis=0, keepdims=True)
    slot = lax.broadcasted_iota(jnp.int32, src.shape, 0) * 128 + lax.broadcasted_iota(jnp.int32, src.shape, 1)
    loads[2].wait()
    live = slot < count[0]
    loads[0].wait()
    into = jnp.where(live, dst[...], 0)
    flags = jnp.take_along_axis(
        jnp.broadcast_to(word, src.shape), lax.bitwise_and(into, 127), axis=1, mode="promise_in_bounds")
    flag = lax.bitwise_and(lax.shift_right_logical(flags, lax.shift_right_logical(into, 7)), 1)
    active = jnp.where(live, flag, 0)
    ahead = jnp.where(iota((depth, depth), 1) < iota((depth, depth), 0), 1.0, 0.0).astype(BF16)
    amount = active.astype(F32)
    rank = dot(ahead, amount.astype(BF16))
    ranks[...] = jnp.where(active > 0, rank, -1.0)
    loads[1].wait()
    packs[...] = src[...] * nodes + into
    longest = jnp.max(jnp.sum(amount, axis=0, keepdims=True)).astype(jnp.int32)
    spots = iota((8, 128), 0)
    held = [jnp.full((8, 128), -1, jnp.int32) for _ in range(depth // 8)]
    for r in range(depth):
        to = jnp.broadcast_to(ranks[r : r + 1, :], (8, 128))
        value = jnp.broadcast_to(packs[r : r + 1, :], (8, 128))
        for b in range(r // 8 + 1):
            held[b] = jnp.where(to == spots + 8.0 * b, value, held[b])
    for b in range(depth // 8):
        dense[8 * b : 8 * b + 8, :] = held[b]

    ladder = iota((block, 128), 0).astype(BF16)

    @pl.loop(0, (longest + group - 1) // group)
    def _(c):
        highs, lows = [], []
        for k in range(group):
            value = dense[pl.ds(c * group + k, 1), :]
            node = jnp.where(value < 0, -1, lax.bitwise_and(value, nodes - 1)).astype(F32)
            marks[:, k * 128 : k * 128 + 128] = jnp.where(index[...] == node, 1.0, 0.0).astype(F8)
            source = lax.shift_right_arithmetic(value, bits)
            highs.append(lax.shift_right_arithmetic(source, block.bit_length() - 1))
            lows.append(lax.bitwise_and(source, block - 1))

        @pl.loop(0, table_rows // (block * unroll))
        def _(outer):
            for inner in range(unroll):
                b = outer * unroll + inner
                hits = []
                for k in range(group):
                    here = jnp.where(highs[k] == b, lows[k], -1).astype(F32).astype(BF16)
                    hits.append(jnp.where(ladder == here, jnp.array(1, BF16), jnp.array(0, BF16)).astype(F8))
                cols = pl.ds(pl.multiple_of(b * block, block), block)
                total[:, cols] += dot(marks[...], jnp.concatenate(hits, axis=1), NT)

    counts[...] = total[...].astype(BF16)


def middle(
    dom, grp, req_len, chunk, block,
    feat, arrived, counts, wanted, halo, w_self, w_neigh, w_hidden, bias, w_out, ends, labels, weight,
    logits, out, g_s, g_n, g_h, g_b, g_o,
    turned, index, feat_w, agg_w, floor, served, received, picks, upper_lower, sums,
    back_sent, back, hidden_sent, hidden_in, hidden_part, hidden_parts, hidden_own, hidden_all,
    small, small_in, small_part, small_parts,
    grad, self_sent, self_in, self_part, self_parts, self_own, self_all,
    neigh_sent, neigh_in, neigh_part, neigh_parts, neigh_own, neigh_all,
    near, far, returned, halo_back,
    s0, r0, s1, r1, s2, r2, *marks,
):
    plane, line = Line("dom", dom), Line("grp", grp)
    in_plane, in_line, all_plane = marks[0:8], marks[8:16], marks[16:22]
    links = Links(dom * grp, grp)
    me = links.me
    nodes, width = feat.shape
    rows, table_rows = counts.shape
    size, parts = row_blocks(rows)
    links.greet()
    index[...] = jnp.broadcast_to(spread_column(wanted[...].astype(F32), req_len), index.shape)
    per = size // req_len
    for i in range(parts):
        span = slice(i * size, i * size + size)
        degree = jnp.sum(counts[span, :].astype(F32), axis=1, keepdims=True)
        floor_deg = jnp.maximum(degree, 1.0)
        total = dot(counts[span, :nodes], feat[...])
        total += dot(counts[span, nodes:], arrived[...].reshape(table_rows - nodes, width))
        agg = (total / floor_deg).astype(BF16)
        own = dot(equal_mask(index[span, :1], iota((size, nodes), 1)), feat[...]).astype(BF16)
        emb = (dot(own, w_self[...]) + dot(agg, w_neigh[...])).astype(BF16)
        served[i * per : i * per + per] = emb.reshape(per, req_len, width)
        feat_w[span, :] = own
        agg_w[span, :] = agg
        floor[span, :] = jnp.broadcast_to(floor_deg, (size, 128))
    links.greeted()
    serve = [(block_of(served), received, s0, r0)]
    links.start(serve)
    received[me] = served[me]
    pairs = ends.shape[1]
    slots = iota((rows, chunk), 0)

    @pl.loop(0, pairs // chunk)
    def _(c):
        span = pl.ds(pl.multiple_of(c * chunk, chunk), chunk)
        end = ends[:, span].astype(F32)
        picks[:rows, span] = equal_mask(slots, end[:1, :])
        picks[rows:, span] = equal_mask(slots, end[1:, :])

    bias_col = column_of(bias[...])
    out_col = column_of(w_out[...])
    sums[...] = jnp.zeros_like(sums)
    links.finish(serve)

    got = received[...].reshape(rows, width)
    for place, half in ((0, w_hidden[:width, :]), (rows, w_hidden[width:, :])):
        exact = dot(got, half).T
        upper = exact.astype(BF16)
        upper_lower[:width, place : place + rows] = upper
        upper_lower[width:, place : place + rows] = (exact - upper.astype(F32)).astype(BF16)

    def step(c, carry):
        bias_sum, out_sum = carry
        span = pl.ds(pl.multiple_of(c * chunk, chunk), chunk)
        both = dot(upper_lower[...], picks[:, span])
        pre = both[:width] + both[width:] + bias_col
        hidden = jnp.maximum(pre, 0.0)
        logit = jnp.sum(hidden * out_col, axis=0, keepdims=True)
        logits[:, span] = logit
        slope = weight[:, span] * (jax.nn.sigmoid(logit) - labels[:, span].astype(F32))
        delta = jnp.where(pre > 0, slope * out_col, 0.0)
        sums[...] += dot(picks[:, span], delta.astype(BF16), NT)
        return (
            bias_sum + jnp.sum(delta, axis=1, keepdims=True),
            out_sum + jnp.sum(hidden * slope, axis=1, keepdims=True),
        )

    zero = jnp.zeros((width, 1), F32)
    bias_sum, out_sum = lax.fori_loop(0, pairs // chunk, step, (zero, zero))
    left = sums[:rows, :].astype(BF16)
    right = sums[rows:, :].astype(BF16)
    back_rows = dot(left, w_hidden[:width, :], NT) + dot(right, w_hidden[width:, :], NT)
    back_sent[...] = back_rows.astype(BF16).reshape(back_sent.shape)
    give = [(block_of(back_sent), back, s1, r1)]
    links.start(give)
    back[me] = back_sent[me]

    small[0:1, :] = row_of(bias_sum)
    small[1:2, :] = row_of(out_sum)
    half = dom // 2
    shape = (half,) + hidden_sent.shape[1:]
    hidden_sent[:half] = dot(got, left, TN).astype(BF16).reshape(shape)
    hidden_sent[half:] = dot(got, right, TN).astype(BF16).reshape(shape)
    hidden_first = [(block_of(hidden_sent), hidden_in) + in_plane[0:2], (whole_of(small), small_in) + in_plane[2:4]]
    plane.start(hidden_first)
    hidden_in[plane.me] = hidden_sent[plane.me]
    small_in[plane.me] = small[...]
    other = row_of(index[:, :1])
    halo_row = row_of(halo_column(halo, turned))
    links.finish(give)

    for i in range(parts):
        span = slice(i * size, i * size + size)
        same = index[span, :1] == other
        first = lax.broadcasted_iota(jnp.int32, same.shape, 0) + i * size
        earlier = lax.broadcasted_iota(jnp.int32, same.shape, 1) < first
        repeat = jnp.sum(jnp.where(same & earlier, 1.0, 0.0), axis=1, keepdims=True)
        total = dot(jnp.where(same, 1.0, 0.0).astype(BF16), back[...].reshape(rows, width))
        grad[span, :] = jnp.where(repeat > 0.0, 0.0, total).astype(BF16)
    self_sent[...] = dot(feat_w[...], grad[...], TN).astype(BF16).reshape(self_sent.shape)
    self_first = [(block_of(self_sent), self_in) + in_plane[4:6]]
    plane.start(self_first)
    neigh_sent[...] = dot(agg_w[...], grad[...], TN).astype(BF16).reshape(neigh_sent.shape)
    neigh_first = [(block_of(neigh_sent), neigh_in) + in_plane[6:8]]
    plane.start(neigh_first)
    self_in[plane.me] = self_sent[plane.me]
    neigh_in[plane.me] = neigh_sent[plane.me]

    far[...] = (dot(grad[...], w_neigh[...], NT) / floor[:, :1]).astype(BF16)
    returned[...] = dot(counts[:, nodes:], far[...], TN).astype(BF16).reshape(returned.shape)
    send_back = [(block_of(returned), halo_back, s2, r2)]
    links.start(send_back)
    halo_back[me] = returned[me]

    plane.finish(hidden_first)
    hidden_part[...] = jnp.sum(hidden_in[...].astype(F32), axis=0).astype(BF16)
    small_part[...] = jnp.sum(small_in[...], axis=0)
    hidden_next = [(whole_of(hidden_part), hidden_parts) + in_line[0:2], (whole_of(small_part), small_parts) + in_line[2:4]]
    line.start(hidden_next)
    hidden_parts[line.me] = hidden_part[...]
    small_parts[line.me] = small_part[...]

    near[...] = dot(grad[...], w_self[...], NT).astype(BF16)

    def local(b, carry):
        cols = pl.ds(pl.multiple_of(b * block, block), block)
        spot = lax.broadcasted_iota(jnp.int32, (1, block), 1) + b * block
        pick = equal_mask(index[:, :1], spot.astype(F32))
        out[cols, :] = dot(counts[:, cols], far[...], TN) + dot(pick, near[...], TN)
        return carry

    lax.fori_loop(0, nodes // block, local, 0)

    plane.finish(self_first)
    self_part[...] = jnp.sum(self_in[...].astype(F32), axis=0).astype(BF16)
    self_next = [(whole_of(self_part), self_parts) + in_line[4:6]]
    line.start(self_next)
    self_parts[line.me] = self_part[...]
    plane.finish(neigh_first)
    neigh_part[...] = jnp.sum(neigh_in[...].astype(F32), axis=0).astype(BF16)
    neigh_next = [(whole_of(neigh_part), neigh_parts) + in_line[6:8]]
    line.start(neigh_next)
    neigh_parts[line.me] = neigh_part[...]

    line.finish(hidden_next)
    hidden_own[...] = jnp.sum(hidden_parts[...].astype(F32), axis=0).astype(BF16)
    hidden_last = [(whole_of(hidden_own), hidden_all) + all_plane[0:2]]
    plane.start(hidden_last)
    hidden_all[plane.me] = hidden_own[...]
    total = jnp.sum(small_parts[...], axis=0)
    g_b[...] = total[0:1, :]
    g_o[...] = total[1:2, :]

    line.finish(self_next)
    self_own[...] = jnp.sum(self_parts[...].astype(F32), axis=0).astype(BF16)
    self_last = [(whole_of(self_own), self_all) + all_plane[2:4]]
    plane.start(self_last)
    self_all[plane.me] = self_own[...]
    line.finish(neigh_next)
    neigh_own[...] = jnp.sum(neigh_parts[...].astype(F32), axis=0).astype(BF16)
    neigh_last = [(whole_of(neigh_own), neigh_all) + all_plane[4:6]]
    plane.start(neigh_last)
    neigh_all[plane.me] = neigh_own[...]

    links.finish(send_back)

    def add(b, carry):
        cols = pl.ds(pl.multiple_of(b * block, block), block)
        spot = iota((block, halo_row.shape[1]), 0) + (b * block).astype(F32)
        out[cols, :] += dot(equal_mask(spot, halo_row), halo_back[...].reshape(halo_row.shape[1], width))
        return carry

    lax.fori_loop(0, nodes // block, add, 0)
    plane.finish(hidden_last)
    g_h[...] = hidden_all[...].astype(F32).reshape(g_h.shape)
    plane.finish(self_last)
    g_s[...] = self_all[...].astype(F32).reshape(g_s.shape)
    plane.finish(neigh_last)
    g_n[...] = neigh_all[...].astype(F32).reshape(g_n.shape)


def put_out(count, *refs):
    sent, kept, done = refs[:count], refs[count : 2 * count], refs[2 * count]
    copies = [pltpu.make_async_copy(src, dst, done.at[i]) for i, (src, dst) in enumerate(zip(sent, kept))]
    for copy in copies:
        copy.start()
    for copy in copies:
        copy.wait()


def store(values):
    count = len(values)
    return pl.pallas_call(
        functools.partial(put_out, count),
        out_shape=tuple(jax.ShapeDtypeStruct(v.shape, v.dtype) for v in values),
        in_specs=[pl.BlockSpec(memory_space=pltpu.VMEM)] * count,
        out_specs=tuple(pl.BlockSpec(memory_space=pl.ANY) for _ in values),
        scratch_shapes=[pltpu.SemaphoreType.DMA((count,))],
        compiler_params=pltpu.CompilerParams(vmem_limit_bytes=8 * 1024 * 1024),
    )(*values)


def row_blocks(rows):
    size = min(rows, 512)
    return size, rows // size


def per_device(
    features, edge_src, edge_dst, edge_count, halo_index, request_rows, pair_ends,
    labels, pair_weight, w_self, w_neigh, w_hidden, b_hidden, w_out,
):
    nodes, width = features.shape
    grp = lax.axis_size("grp")
    dom = lax.axis_size("dom")
    peers = dom * grp
    halo_len = halo_index.shape[2]
    req_len = request_rows.shape[2]
    slots = edge_src.shape[0]
    pairs = labels.shape[0]
    table_rows = nodes + peers * halo_len
    rows = peers * req_len
    block = 256
    piece = width // dom
    turn = max(128, peers)

    halo = halo_index[0].T
    wanted, arrived = call(
        functools.partial(first_exchange, peers, grp),
        [((peers, 1, 128), jnp.int32), ((peers, halo_len, width), BF16)],
        (features, halo, request_rows[0].T),
        [
            pltpu.VMEM((nodes, width), BF16),
            pltpu.VMEM((halo_len, peers), jnp.int32),
            pltpu.VMEM((req_len, peers), jnp.int32),
            pltpu.SemaphoreType.DMA((3,)),
            pltpu.VMEM((128, turn), F32),
            pltpu.VMEM((peers, 1, 128), jnp.int32),
            pltpu.VMEM((peers, halo_len, width), BF16),
        ] + sems(peers, 2),
        collective_id=0,
        hbm=(0, 1, 2),
        limit=K1LIM,
        micros=10,
    )
    group = GROUP
    depth = slots // 128
    (counts,) = call(
        functools.partial(count_edges, req_len, nodes, block, group, table_rows // block),
        [((rows, table_rows), BF16)],
        (edge_src.reshape(depth, 128), edge_dst.reshape(depth, 128), edge_count, wanted),
        [
            pltpu.VMEM((depth, 128), jnp.int32),
            pltpu.VMEM((depth, 128), jnp.int32),
            pltpu.SMEM((1,), jnp.int32),
            pltpu.SemaphoreType.DMA((3,)),
            pltpu.VMEM((rows, table_rows), F32),
            pltpu.VMEM((rows, group * 128), F8),
            pltpu.VMEM((rows, 128), F32),
            pltpu.VMEM((depth, 128), F32),
            pltpu.VMEM((depth, 128), jnp.int32),
            pltpu.VMEM((depth, 128), jnp.int32),
        ],
        hbm=(0, 1, 2),
        limit=min(VMEM_LIMIT, rows * 40 * 1024),
    )
    chunk = 512
    rows_of = lambda *shape: pltpu.VMEM(shape, BF16)
    found = call(
        functools.partial(middle, dom, grp, req_len, chunk, block),
        [
            ((1, pairs), F32),
            ((nodes, width), F32),
            ((width, width), F32),
            ((width, width), F32),
            ((2 * width, width), F32),
            ((1, width), F32),
            ((1, width), F32),
        ],
        (
            features, arrived, counts, wanted, halo, w_self, w_neigh, w_hidden,
            b_hidden.reshape(1, width), w_out.reshape(1, width),
            pair_ends.T, labels.reshape(1, pairs), pair_weight.reshape(1, pairs),
        ),
        [
            pltpu.VMEM((128, turn), F32),
            pltpu.VMEM((rows, 128), F32),
            rows_of(rows, width),
            rows_of(rows, width),
            pltpu.VMEM((rows, 128), F32),
            rows_of(peers, req_len, width),
            rows_of(peers, req_len, width),
            rows_of(2 * rows, pairs),
            rows_of(2 * width, 2 * rows),
            pltpu.VMEM((2 * rows, width), F32),
            rows_of(peers, req_len, width),
            rows_of(peers, req_len, width),
            rows_of(dom, 2 * piece, width),
            rows_of(dom, 2 * piece, width),
            rows_of(2 * piece, width),
            rows_of(grp, 2 * piece, width),
            rows_of(2 * piece, width),
            rows_of(dom, 2 * piece, width),
            pltpu.VMEM((2, width), F32),
            pltpu.VMEM((dom, 2, width), F32),
            pltpu.VMEM((2, width), F32),
            pltpu.VMEM((grp, 2, width), F32),
            rows_of(rows, width),
        ] + 2 * [
            rows_of(dom, piece, width),
            rows_of(dom, piece, width),
            rows_of(piece, width),
            rows_of(grp, piece, width),
            rows_of(piece, width),
            rows_of(dom, piece, width),
        ] + [
            rows_of(rows, width),
            rows_of(rows, width),
            rows_of(peers, halo_len, width),
            rows_of(peers, halo_len, width),
        ] + sems(peers, 3) + sems(dom, 4) + sems(grp, 4) + sems(dom, 3),
        collective_id=1,
        limit=min(VMEM_LIMIT, rows * 60 * 1024),
    )
    logits, grad_features, g_s, g_n, g_h, g_b, g_o = store(found)
    return (logits.reshape(pairs), grad_features, g_s, g_n, g_h, g_b.reshape(width), g_o.reshape(width))


def solution(mesh):
    both = ("dom", "grp")
    in_specs = (
        P(both, None), P(both), P(both), P(both), P(both, None, None), P(both, None, None),
        P(both, None), P(both), P(both), P(), P(), P(), P(), P(),
    )
    out_specs = (P(both), P(both, None), P(), P(), P(), P(), P())
    return jax.shard_map(
        per_device, mesh=mesh, in_specs=in_specs, out_specs=out_specs, check_vma=False
    )
```

```python
import functools

import jax
import jax.numpy as jnp
from jax import lax
from jax.experimental import pallas as pl
from jax.experimental.pallas import tpu as pltpu
from jax.sharding import PartitionSpec as P

F32 = jnp.float32
BF16 = jnp.bfloat16
F8 = jnp.float8_e4m3fn
VMEM_LIMIT = 63 * 1024 * 1024
K1LIM = 64 * 1024 * 1024 - 512 * 1024
NN = (((1,), (0,)), ((), ()))
NT = (((1,), (1,)), ((), ()))
TN = (((0,), (0,)), ((), ()))


def dot(left, right, dims=NN):
    return lax.dot_general(left, right, dims, preferred_element_type=F32)


def column_of(row):
    return jnp.broadcast_to(row, (128, row.shape[1])).T[:, :1]


def row_of(column):
    return jnp.broadcast_to(column, (column.shape[0], 128)).T[:1, :]


def equal_mask(left, right):
    return jnp.where(left == right, 1.0, 0.0).astype(BF16)


def iota(shape, dim):
    return lax.broadcasted_iota(jnp.int32, shape, dim).astype(F32)


class Links:
    def __init__(self, peers, grp):
        self.peers, self.grp = peers, grp
        self.me = lax.axis_index("dom") * grp + lax.axis_index("grp")

    def device(self, peer):
        return {"dom": peer // self.grp, "grp": lax.rem(peer, self.grp)}

    def other(self, step):
        return lax.rem(self.me + step, self.peers)

    def each(self, body):
        def step(i, carry):
            body(self.other(i))
            return carry

        lax.fori_loop(1, self.peers, step, 0)

    def greet(self):
        barrier = pltpu.get_barrier_semaphore()
        self.each(lambda peer: pl.semaphore_signal(
            barrier, inc=1, device_id=self.device(peer), device_id_type=pl.DeviceIdType.MESH))

    def greeted(self):
        pl.semaphore_wait(pltpu.get_barrier_semaphore(), self.peers - 1)

    def copy(self, src, dst, send, recv, peer, slot):
        return pltpu.make_async_remote_copy(
            src_ref=src, dst_ref=dst, send_sem=send.at[peer], recv_sem=recv.at[slot],
            device_id=self.device(peer), device_id_type=pl.DeviceIdType.MESH)

    def start(self, moves):
        def one(peer):
            for pick, dst, send, recv in moves:
                self.copy(pick(peer), dst.at[self.me], send, recv, peer, self.me).start()

        self.each(one)

    def finish(self, moves):
        def one(peer):
            for pick, dst, send, recv in moves:
                copy = self.copy(pick(peer), dst.at[peer], send, recv, peer, peer)
                copy.wait_recv()
                copy.wait_send()

        self.each(one)


class Line(Links):
    def __init__(self, axis, peers):
        self.axis, self.peers = axis, peers
        self.me = lax.axis_index(axis)

    def device(self, peer):
        return {self.axis: peer}


def block_of(ref):
    return lambda peer: ref.at[peer]


def whole_of(ref):
    return lambda peer: ref


def sems(peers, count):
    return [pltpu.SemaphoreType.DMA((peers,)) for _ in range(2 * count)]


def call(body, outs, args, scratch=(), collective_id=None, hbm=(), limit=VMEM_LIMIT, micros=0):
    params = dict(vmem_limit_bytes=limit)
    if collective_id is not None:
        params.update(collective_id=collective_id, has_side_effects=True)
    return pl.pallas_call(
        body,
        out_shape=tuple(jax.ShapeDtypeStruct(s, d) for s, d in outs),
        in_specs=[
            pl.BlockSpec(memory_space=pltpu.HBM if i in hbm else pltpu.VMEM)
            for i in range(len(args))
        ],
        out_specs=tuple(pl.BlockSpec(memory_space=pltpu.VMEM) for _ in outs),
        scratch_shapes=list(scratch),
        compiler_params=pltpu.CompilerParams(**params),
        cost_estimate=pl.CostEstimate(flops=micros * 10**9, bytes_accessed=1024, transcendentals=0) if micros else None,
    )(*args)


def spread_column(rows, length):
    peers = rows.shape[0]
    spread = jnp.broadcast_to(rows, (peers, length, 128)).reshape(peers * length, 128)
    lane = lax.broadcasted_iota(jnp.int32, spread.shape, 1)
    row = lax.rem(lax.broadcasted_iota(jnp.int32, spread.shape, 0), length)
    return jnp.sum(jnp.where(lane == row, spread, 0.0), axis=1, keepdims=True)


def halo_column(halo, turned):
    halo_len, peers = halo.shape
    turned[...] = jnp.zeros_like(turned)
    turned[:halo_len, :peers] = halo[...].astype(F32)
    return spread_column(turned[...].T[:peers].reshape(peers, 1, 128), halo_len)


def fetch(pairs, done):
    return [pltpu.make_async_copy(src, dst, done.at[i]) for i, (src, dst) in enumerate(pairs)]


def first_exchange(
    peers, grp, feat_far, halo_far, request_far, wanted, arrived,
    feat, halo, request, done, turned, asked, outgoing, s0, r0, s1, r1,
):
    links = Links(peers, grp)
    me = links.me
    loads = fetch([(request_far, request), (halo_far, halo), (feat_far, feat)], done)
    for load in loads:
        load.start()
    links.greet()
    nodes = feat.shape[0]
    loads[0].wait()
    loads[1].wait()
    turned[...] = jnp.zeros_like(turned)
    turned[: request.shape[0], :peers] = request[...].astype(F32)
    asked[...] = turned[...].T[:peers].astype(jnp.int32).reshape(asked.shape)
    index = halo_column(halo, turned)
    pick = equal_mask(index, iota((index.shape[0], nodes), 1))
    loads[2].wait()
    outgoing[...] = dot(pick, feat[...]).astype(BF16).reshape(outgoing.shape)
    links.greeted()
    moves = [(block_of(asked), wanted, s0, r0), (block_of(outgoing), arrived, s1, r1)]
    links.start(moves)
    wanted[me] = asked[me]
    arrived[me] = outgoing[me]
    links.finish(moves)


def mark_edges(values, index, marks, nodes, block):
    highs, lows = [], []
    for k, value in enumerate(values):
        node = jnp.where(value < 0, -1, lax.bitwise_and(value, nodes - 1)).astype(F32)
        marks[:, k * 128 : k * 128 + 128] = jnp.where(index[...] == node, 1.0, 0.0).astype(F8)
        source = lax.shift_right_arithmetic(value, nodes.bit_length() - 1)
        highs.append(lax.shift_right_arithmetic(source, block.bit_length() - 1))
        lows.append(lax.bitwise_and(source, block - 1))
    ladder = iota((block, 128), 0).astype(BF16)

    def count(b):
        hits = []
        for high, low in zip(highs, lows):
            here = jnp.where(high == b, low, -1).astype(F32).astype(BF16)
            hits.append(jnp.where(ladder == here, jnp.array(1, BF16), jnp.array(0, BF16)).astype(F8))
        return dot(marks[...], jnp.concatenate(hits, axis=1), NT)

    return count


def count_edges(
    req_len, nodes, block, group, merge, early, src_far, dst_far, count_far, wanted, counts, head,
    src, dst, count, done, total, marks, index, ranks, packs, dense,
):
    loads = fetch([(dst_far, dst), (src_far, src), (count_far, count)], done)
    for load in loads:
        load.start()
    rows, table_rows = counts.shape
    depth = src.shape[0]
    total[...] = jnp.zeros_like(total)
    column = spread_column(wanted[...].astype(F32), req_len)
    index[...] = jnp.broadcast_to(column, index.shape)
    high = jnp.floor(column * (1.0 / 128.0))
    low = column - high * 128.0
    lanes = iota((rows, 128), 1)
    seen = dot(equal_mask(high, lanes), equal_mask(low, lanes), TN)[: nodes // 128]
    power = lax.shift_left(jnp.ones(seen.shape, jnp.int32), lax.broadcasted_iota(jnp.int32, seen.shape, 0))
    word = jnp.sum(jnp.where(seen > 0.5, power, 0), axis=0, keepdims=True)
    lane = lax.broadcasted_iota(jnp.int32, src.shape, 1)
    slot = lax.broadcasted_iota(jnp.int32, src.shape, 0) * 128 + lane
    loads[2].wait()
    live = slot < count[0]
    loads[0].wait()
    into = jnp.where(live, dst[...], 0)
    flags = jnp.take_along_axis(
        jnp.broadcast_to(word, src.shape), lax.bitwise_and(into, 127), axis=1, mode="promise_in_bounds")
    flag = lax.bitwise_and(lax.shift_right_logical(flags, lax.shift_right_logical(into, 7)), 1)
    active = jnp.where(live, flag, 0).astype(F32)
    stride = 128 // merge
    ahead = jnp.where(iota((depth, depth), 1) < iota((depth, depth), 0), 1.0, 0.0).astype(BF16)
    group_sum = active
    before = jnp.zeros_like(active)
    for d in range(1, merge):
        turned = pltpu.roll(active, d * stride, 1)
        group_sum = group_sum + turned
        before = before + jnp.where(lane >= d * stride, turned, 0.0)
    rank = dot(ahead, group_sum.astype(BF16)) + before
    spot = jnp.floor(rank * (1.0 / merge))
    moved = rank - spot * merge - (lane // stride).astype(F32)
    moved = jnp.where(moved < 0.0, moved + merge, moved)
    loads[1].wait()
    pack = src[...] * nodes + into
    for d in range(merge):
        goes = jnp.where((active > 0.5) & (moved == d), spot, -1.0)
        ranks[d] = pltpu.roll(goes, d * stride, 1) if d else goes
        packs[d] = pltpu.roll(pack, d * stride, 1) if d else pack
    most = jnp.max(jnp.sum(group_sum, axis=0, keepdims=True)).astype(jnp.int32)
    longest = (most + merge - 1) // merge
    steps = iota((8, 128), 0)
    for b in range(depth // 8):
        @pl.when((b * 8 < longest) | (b * 8 < early * group))
        def _():
            held = jnp.full((8, 128), -1, jnp.int32)
            for r in range(8 * b, depth):
                for d in range(merge):
                    to = jnp.broadcast_to(ranks[d, r : r + 1, :], (8, 128))
                    value = jnp.broadcast_to(packs[d, r : r + 1, :], (8, 128))
                    held = jnp.where(to == steps + 8.0 * b, value, held)
            dense[8 * b : 8 * b + 8, :] = held
    head[...] = dense[: head.shape[0], :]

    @pl.loop(early, (longest + group - 1) // group)
    def _(c):
        values = [dense[pl.ds(c * group + k, 1), :] for k in range(group)]
        count_block = mark_edges(values, index, marks, nodes, block)
        for b in range(table_rows // block):
            total[:, b * block : b * block + block] += count_block(b)

    counts[...] = total[...].astype(BF16)


def middle(
    dom, grp, req_len, chunk, block, early,
    feat, arrived, counted, head, wanted, halo, w_self, w_neigh, w_hidden, bias, w_out, ends, labels, weight,
    logits, out, g_s, g_n, g_h, g_b, g_o,
    turned, index, feat_w, agg_w, floor, served, received, picks, upper_lower, deltas,
    back_sent, back, hidden_sent, hidden_in, hidden_part, hidden_pieces, hidden_piece, hidden_own, hidden_all,
    small, small_in, small_part, small_parts,
    grad, self_sent, self_in, self_part, self_parts, self_own, self_all,
    neigh_sent, neigh_in, neigh_part, neigh_parts, neigh_own, neigh_all,
    near, far, returned, halo_back, feat_t, agg_t,
    s0, r0, s1, r1, s2, r2, *more,
):
    plane, line = Line("dom", dom), Line("grp", grp)
    in_plane, in_line, all_plane, extra = more[0:8], more[8:18], more[18:24], more[24:]
    links = Links(dom * grp, grp)
    me = links.me
    nodes, width = feat.shape
    rows, table_rows = counted.shape
    size, parts = row_blocks(rows)
    links.greet()
    index[...] = jnp.broadcast_to(spread_column(wanted[...].astype(F32), req_len), index.shape)
    per = size // req_len
    counts = counted
    if early:
        counts, edge_marks = extra
        values = [head[k : k + 1, :] for k in range(head.shape[0])]
        count_block = mark_edges(values, index, edge_marks, nodes, block)
        for b in range(table_rows // block):
            cols = slice(b * block, b * block + block)
            counts[:, cols] = (counted[:, cols].astype(F32) + count_block(b)).astype(BF16)
    for i in range(parts):
        span = slice(i * size, i * size + size)
        degree = jnp.sum(counts[span, :].astype(F32), axis=1, keepdims=True)
        floor_deg = jnp.maximum(degree, 1.0)
        total = dot(counts[span, :nodes], feat[...])
        total += dot(counts[span, nodes:], arrived[...].reshape(table_rows - nodes, width))
        agg = (total / floor_deg).astype(BF16)
        own = dot(equal_mask(index[span, :1], iota((size, nodes), 1)), feat[...]).astype(BF16)
        emb = (dot(own, w_self[...]) + dot(agg, w_neigh[...])).astype(BF16)
        served[i * per : i * per + per] = emb.reshape(per, req_len, width)
        feat_w[span, :] = own
        agg_w[span, :] = agg
        floor[span, :] = jnp.broadcast_to(floor_deg, (size, 128))
    links.greeted()
    serve = [(block_of(served), received, s0, r0)]
    links.start(serve)
    received[me] = served[me]
    pairs = ends.shape[1]
    slots = iota((rows, chunk), 0)

    @pl.loop(0, pairs // chunk)
    def _(c):
        span = pl.ds(pl.multiple_of(c * chunk, chunk), chunk)
        end = ends[:, span].astype(F32)
        picks[:rows, span] = equal_mask(slots, end[:1, :])
        picks[rows:, span] = equal_mask(slots, end[1:, :])

    bias_col = column_of(bias[...])
    out_col = column_of(w_out[...])
    links.finish(serve)

    got = received[...].reshape(rows, width)
    for place, half in ((0, w_hidden[:width, :]), (rows, w_hidden[width:, :])):
        exact = dot(got, half).T
        upper = exact.astype(BF16)
        upper_lower[:width, place : place + rows] = upper
        upper_lower[width:, place : place + rows] = (exact - upper.astype(F32)).astype(BF16)

    def step(c, carry):
        bias_sum, out_sum = carry
        span = pl.ds(pl.multiple_of(c * chunk, chunk), chunk)
        both = dot(upper_lower[...], picks[:, span])
        pre = both[:width] + both[width:] + bias_col
        hidden = jnp.maximum(pre, 0.0)
        logit = jnp.sum(hidden * out_col, axis=0, keepdims=True)
        logits[:, span] = logit
        slope = weight[:, span] * (jax.nn.sigmoid(logit) - labels[:, span].astype(F32))
        delta = jnp.where(pre > 0, slope * out_col, 0.0)
        deltas[:, span] = delta.astype(BF16)
        return (
            bias_sum + jnp.sum(delta, axis=1, keepdims=True),
            out_sum + jnp.sum(hidden * slope, axis=1, keepdims=True),
        )

    zero = jnp.zeros((width, 1), F32)
    bias_sum, out_sum = lax.fori_loop(0, pairs // chunk, step, (zero, zero), unroll=True)
    left = dot(picks[:rows, :], deltas[...], NT).astype(BF16)
    right = dot(picks[rows:, :], deltas[...], NT).astype(BF16)
    back_rows = dot(left, w_hidden[:width, :], NT) + dot(right, w_hidden[width:, :], NT)
    back_sent[...] = back_rows.astype(BF16).reshape(back_sent.shape)
    give = [(block_of(back_sent), back, s1, r1)]
    links.start(give)
    back[me] = back_sent[me]

    small[0:1, :] = row_of(bias_sum)
    small[1:2, :] = row_of(out_sum)
    half = dom // 2
    shape = (half,) + hidden_sent.shape[1:]
    hidden_sent[:half] = dot(got, left, TN).astype(BF16).reshape(shape)
    hidden_sent[half:] = dot(got, right, TN).astype(BF16).reshape(shape)
    hidden_first = [(block_of(hidden_sent), hidden_in) + in_plane[0:2], (whole_of(small), small_in) + in_plane[2:4]]
    plane.start(hidden_first)
    hidden_in[plane.me] = hidden_sent[plane.me]
    small_in[plane.me] = small[...]
    other = row_of(index[:, :1])
    halo_row = row_of(halo_column(halo, turned))
    feat_t[...] = feat_w[...].T
    agg_t[...] = agg_w[...].T
    plane.finish(hidden_first)
    hidden_part[...] = jnp.sum(hidden_in[...].astype(F32), axis=0).astype(BF16).reshape(hidden_part.shape)
    small_part[...] = jnp.sum(small_in[...], axis=0)
    hidden_second = [
        (block_of(hidden_part), hidden_pieces) + in_line[0:2],
        (whole_of(small_part), small_parts) + in_line[2:4],
    ]
    line.start(hidden_second)
    hidden_pieces[line.me] = hidden_part[line.me]
    small_parts[line.me] = small_part[...]
    links.finish(give)

    back_all = back[...].reshape(rows, width)
    self_sent[...] = dot(feat_t[...], back_all).astype(BF16).reshape(self_sent.shape)
    self_first = [(block_of(self_sent), self_in) + in_plane[4:6]]
    plane.start(self_first)
    neigh_sent[...] = dot(agg_t[...], back_all).astype(BF16).reshape(neigh_sent.shape)
    neigh_first = [(block_of(neigh_sent), neigh_in) + in_plane[6:8]]
    plane.start(neigh_first)
    for i in range(parts):
        span = slice(i * size, i * size + size)
        same = index[span, :1] == other
        first = lax.broadcasted_iota(jnp.int32, same.shape, 0) + i * size
        earlier = lax.broadcasted_iota(jnp.int32, same.shape, 1) < first
        repeat = jnp.sum(jnp.where(same & earlier, 1.0, 0.0), axis=1, keepdims=True)
        total = dot(jnp.where(same, 1.0, 0.0).astype(BF16), back_all)
        grad[span, :] = jnp.where(repeat > 0.0, 0.0, total).astype(BF16)
    far[...] = (dot(grad[...], w_neigh[...], NT) / floor[:, :1]).astype(BF16)
    returned[...] = dot(counts[:, nodes:], far[...], TN).astype(BF16).reshape(returned.shape)
    send_back = [(block_of(returned), halo_back, s2, r2)]
    links.start(send_back)
    halo_back[me] = returned[me]
    self_in[plane.me] = self_sent[plane.me]
    neigh_in[plane.me] = neigh_sent[plane.me]

    line.finish(hidden_second)
    hidden_piece[...] = jnp.sum(hidden_pieces[...].astype(F32), axis=0).astype(BF16)
    hidden_third = [(whole_of(hidden_piece), hidden_own) + in_line[4:6]]
    line.start(hidden_third)
    hidden_own[line.me] = hidden_piece[...]
    total = jnp.sum(small_parts[...], axis=0)
    g_b[...] = total[0:1, :]
    g_o[...] = total[1:2, :]
    near[...] = dot(grad[...], w_self[...], NT).astype(BF16)

    def local(b, carry):
        cols = pl.ds(pl.multiple_of(b * block, block), block)
        spot = lax.broadcasted_iota(jnp.int32, (1, block), 1) + b * block
        pick = equal_mask(index[:, :1], spot.astype(F32))
        out[cols, :] = dot(counts[:, cols], far[...], TN) + dot(pick, near[...], TN)
        return carry

    cut = nodes // block * 5 // 8
    lax.fori_loop(0, cut, local, 0)
    plane.finish(self_first)
    self_part[...] = jnp.sum(self_in[...].astype(F32), axis=0).astype(BF16)
    self_next = [(whole_of(self_part), self_parts) + in_line[6:8]]
    line.start(self_next)
    self_parts[line.me] = self_part[...]
    lax.fori_loop(cut, nodes // block, local, 0)
    plane.finish(neigh_first)
    neigh_part[...] = jnp.sum(neigh_in[...].astype(F32), axis=0).astype(BF16)
    neigh_next = [(whole_of(neigh_part), neigh_parts) + in_line[8:10]]
    line.start(neigh_next)
    neigh_parts[line.me] = neigh_part[...]

    line.finish(hidden_third)
    hidden_last = [(whole_of(hidden_own), hidden_all) + all_plane[0:2]]
    plane.start(hidden_last)
    hidden_all[plane.me] = hidden_own[...]

    links.finish(send_back)

    def add(b, carry):
        cols = pl.ds(pl.multiple_of(b * block, block), block)
        spot = iota((block, halo_row.shape[1]), 0) + (b * block).astype(F32)
        out[cols, :] += dot(equal_mask(spot, halo_row), halo_back[...].reshape(halo_row.shape[1], width))
        return carry

    lax.fori_loop(0, nodes // block, add, 0)
    line.finish(self_next)
    self_own[...] = jnp.sum(self_parts[...].astype(F32), axis=0).astype(BF16)
    self_last = [(whole_of(self_own), self_all) + all_plane[2:4]]
    plane.start(self_last)
    self_all[plane.me] = self_own[...]
    line.finish(neigh_next)
    neigh_own[...] = jnp.sum(neigh_parts[...].astype(F32), axis=0).astype(BF16)
    neigh_last = [(whole_of(neigh_own), neigh_all) + all_plane[4:6]]
    plane.start(neigh_last)
    neigh_all[plane.me] = neigh_own[...]
    plane.finish(hidden_last)
    g_h[...] = hidden_all[...].astype(F32).reshape(g_h.shape)
    plane.finish(self_last)
    g_s[...] = self_all[...].astype(F32).reshape(g_s.shape)
    plane.finish(neigh_last)
    g_n[...] = neigh_all[...].astype(F32).reshape(g_n.shape)


def put_out(count, *refs):
    sent, kept, done = refs[:count], refs[count : 2 * count], refs[2 * count]
    copies = [pltpu.make_async_copy(src, dst, done.at[i]) for i, (src, dst) in enumerate(zip(sent, kept))]
    for copy in copies:
        copy.start()
    for copy in copies:
        copy.wait()


def store(values):
    count = len(values)
    return pl.pallas_call(
        functools.partial(put_out, count),
        out_shape=tuple(jax.ShapeDtypeStruct(v.shape, v.dtype) for v in values),
        in_specs=[pl.BlockSpec(memory_space=pltpu.VMEM)] * count,
        out_specs=tuple(pl.BlockSpec(memory_space=pl.ANY) for _ in values),
        scratch_shapes=[pltpu.SemaphoreType.DMA((count,))],
        compiler_params=pltpu.CompilerParams(vmem_limit_bytes=8 * 1024 * 1024),
    )(*values)


def row_blocks(rows):
    size = min(rows, 512)
    return size, rows // size


def per_device(
    features, edge_src, edge_dst, edge_count, halo_index, request_rows, pair_ends,
    labels, pair_weight, w_self, w_neigh, w_hidden, b_hidden, w_out,
):
    nodes, width = features.shape
    grp = lax.axis_size("grp")
    dom = lax.axis_size("dom")
    peers = dom * grp
    halo_len = halo_index.shape[2]
    req_len = request_rows.shape[2]
    slots = edge_src.shape[0]
    pairs = labels.shape[0]
    table_rows = nodes + peers * halo_len
    rows = peers * req_len
    block = 256
    piece = width // dom
    turn = max(128, peers)

    halo = halo_index[0].T
    wanted, arrived = call(
        functools.partial(first_exchange, peers, grp),
        [((peers, 1, 128), jnp.int32), ((peers, halo_len, width), BF16)],
        (features, halo, request_rows[0].T),
        [
            pltpu.VMEM((nodes, width), BF16),
            pltpu.VMEM((halo_len, peers), jnp.int32),
            pltpu.VMEM((req_len, peers), jnp.int32),
            pltpu.SemaphoreType.DMA((3,)),
            pltpu.VMEM((128, turn), F32),
            pltpu.VMEM((peers, 1, 128), jnp.int32),
            pltpu.VMEM((peers, halo_len, width), BF16),
        ] + sems(peers, 2),
        collective_id=0,
        hbm=(0, 1, 2),
        limit=K1LIM,
        micros=10,
    )
    group = 8
    depth = slots // 128
    merge = 2
    early = 1 if rows <= 1024 else 0
    counts, head = call(
        functools.partial(count_edges, req_len, nodes, block, group, merge, early),
        [((rows, table_rows), BF16), ((group, 128), jnp.int32)],
        (edge_src.reshape(depth, 128), edge_dst.reshape(depth, 128), edge_count, wanted),
        [
            pltpu.VMEM((depth, 128), jnp.int32),
            pltpu.VMEM((depth, 128), jnp.int32),
            pltpu.SMEM((1,), jnp.int32),
            pltpu.SemaphoreType.DMA((3,)),
            pltpu.VMEM((rows, table_rows), F32),
            pltpu.VMEM((rows, group * 128), F8),
            pltpu.VMEM((rows, 128), F32),
            pltpu.VMEM((merge, depth, 128), F32),
            pltpu.VMEM((merge, depth, 128), jnp.int32),
            pltpu.VMEM((depth, 128), jnp.int32),
        ],
        hbm=(0, 1, 2),
        micros=10,
        limit=min(VMEM_LIMIT, rows * 40 * 1024),
    )
    chunk = 512
    rows_of = lambda *shape: pltpu.VMEM(shape, BF16)
    found = call(
        functools.partial(middle, dom, grp, req_len, chunk, block, early),
        [
            ((1, pairs), F32),
            ((nodes, width), F32),
            ((width, width), F32),
            ((width, width), F32),
            ((2 * width, width), F32),
            ((1, width), F32),
            ((1, width), F32),
        ],
        (
            features, arrived, counts, head, wanted, halo, w_self, w_neigh, w_hidden,
            b_hidden.reshape(1, width), w_out.reshape(1, width),
            pair_ends.T, labels.reshape(1, pairs), pair_weight.reshape(1, pairs),
        ),
        [
            pltpu.VMEM((128, turn), F32),
            pltpu.VMEM((rows, 128), F32),
            rows_of(rows, width),
            rows_of(rows, width),
            pltpu.VMEM((rows, 128), F32),
            rows_of(peers, req_len, width),
            rows_of(peers, req_len, width),
            rows_of(2 * rows, pairs),
            rows_of(2 * width, 2 * rows),
            rows_of(width, pairs),
            rows_of(peers, req_len, width),
            rows_of(peers, req_len, width),
            rows_of(dom, 2 * piece, width),
            rows_of(dom, 2 * piece, width),
            rows_of(grp, 2 * piece // grp, width),
            rows_of(grp, 2 * piece // grp, width),
            rows_of(2 * piece // grp, width),
            rows_of(grp, 2 * piece // grp, width),
            rows_of(dom, grp, 2 * piece // grp, width),
            pltpu.VMEM((2, width), F32),
            pltpu.VMEM((dom, 2, width), F32),
            pltpu.VMEM((2, width), F32),
            pltpu.VMEM((grp, 2, width), F32),
            rows_of(rows, width),
        ] + 2 * [
            rows_of(dom, piece, width),
            rows_of(dom, piece, width),
            rows_of(piece, width),
            rows_of(grp, piece, width),
            rows_of(piece, width),
            rows_of(dom, piece, width),
        ] + [
            rows_of(rows, width),
            rows_of(rows, width),
            rows_of(peers, halo_len, width),
            rows_of(peers, halo_len, width),
            rows_of(width, rows),
            rows_of(width, rows),
        ] + sems(peers, 3) + sems(dom, 4) + sems(grp, 5) + sems(dom, 3) + early * [rows_of(rows, table_rows), pltpu.VMEM((rows, group * 128), F8)],
        collective_id=1,
        limit=min(VMEM_LIMIT, rows * 60 * 1024),
    )
    logits, grad_features, g_s, g_n, g_h, g_b, g_o = store(found)
    return (logits.reshape(pairs), grad_features, g_s, g_n, g_h, g_b.reshape(width), g_o.reshape(width))


def solution(mesh):
    both = ("dom", "grp")
    in_specs = (
        P(both, None), P(both), P(both), P(both), P(both, None, None), P(both, None, None),
        P(both, None), P(both), P(both), P(), P(), P(), P(), P(),
    )
    out_specs = (P(both), P(both, None), P(), P(), P(), P(), P())
    return jax.shard_map(
        per_device, mesh=mesh, in_specs=in_specs, out_specs=out_specs, check_vma=False
    )
```

```python
import functools

import jax
import jax.numpy as jnp
from jax import lax
from jax.experimental import pallas as pl
from jax.experimental.pallas import tpu as pltpu
from jax.sharding import PartitionSpec as P

F32 = jnp.float32
BF16 = jnp.bfloat16
F8 = jnp.float8_e4m3fn
VMEM_LIMIT = 63 * 1024 * 1024
K1LIM = 64 * 1024 * 1024 - 512 * 1024
NN = (((1,), (0,)), ((), ()))
NT = (((1,), (1,)), ((), ()))
TN = (((0,), (0,)), ((), ()))


def dot(left, right, dims=NN):
    return lax.dot_general(left, right, dims, preferred_element_type=F32)


def column_of(row):
    return jnp.broadcast_to(row, (128, row.shape[1])).T[:, :1]


def row_of(column):
    return jnp.broadcast_to(column, (column.shape[0], 128)).T[:1, :]


def equal_mask(left, right):
    return jnp.where(left == right, 1.0, 0.0).astype(BF16)


def iota(shape, dim):
    return lax.broadcasted_iota(jnp.int32, shape, dim).astype(F32)


class Links:
    def __init__(self, peers, grp):
        self.peers, self.grp = peers, grp
        self.me = lax.axis_index("dom") * grp + lax.axis_index("grp")

    def device(self, peer):
        return {"dom": peer // self.grp, "grp": lax.rem(peer, self.grp)}

    def other(self, step):
        return lax.rem(self.me + step, self.peers)

    def each(self, body):
        def step(i, carry):
            body(self.other(i))
            return carry

        lax.fori_loop(1, self.peers, step, 0)

    def greet(self):
        barrier = pltpu.get_barrier_semaphore()
        self.each(lambda peer: pl.semaphore_signal(
            barrier, inc=1, device_id=self.device(peer), device_id_type=pl.DeviceIdType.MESH))

    def greeted(self):
        pl.semaphore_wait(pltpu.get_barrier_semaphore(), self.peers - 1)

    def copy(self, src, dst, send, recv, peer, slot):
        return pltpu.make_async_remote_copy(
            src_ref=src, dst_ref=dst, send_sem=send.at[peer], recv_sem=recv.at[slot],
            device_id=self.device(peer), device_id_type=pl.DeviceIdType.MESH)

    def start(self, moves):
        def one(peer):
            for pick, dst, send, recv in moves:
                self.copy(pick(peer), dst.at[self.me], send, recv, peer, self.me).start()

        self.each(one)

    def finish(self, moves):
        def one(peer):
            for pick, dst, send, recv in moves:
                copy = self.copy(pick(peer), dst.at[peer], send, recv, peer, peer)
                copy.wait_recv()
                copy.wait_send()

        self.each(one)


class Line(Links):
    def __init__(self, axis, peers):
        self.axis, self.peers = axis, peers
        self.me = lax.axis_index(axis)

    def device(self, peer):
        return {self.axis: peer}


def block_of(ref):
    return lambda peer: ref.at[peer]


def whole_of(ref):
    return lambda peer: ref


def sems(peers, count):
    return [pltpu.SemaphoreType.DMA((peers,)) for _ in range(2 * count)]


def call(body, outs, args, scratch=(), collective_id=None, hbm=(), limit=VMEM_LIMIT, micros=0):
    params = dict(vmem_limit_bytes=limit)
    if collective_id is not None:
        params.update(collective_id=collective_id, has_side_effects=True)
    return pl.pallas_call(
        body,
        out_shape=tuple(jax.ShapeDtypeStruct(s, d) for s, d in outs),
        in_specs=[
            pl.BlockSpec(memory_space=pltpu.HBM if i in hbm else pltpu.VMEM)
            for i in range(len(args))
        ],
        out_specs=tuple(pl.BlockSpec(memory_space=pltpu.VMEM) for _ in outs),
        scratch_shapes=list(scratch),
        compiler_params=pltpu.CompilerParams(**params),
        cost_estimate=pl.CostEstimate(flops=micros * 10**9, bytes_accessed=1024, transcendentals=0) if micros else None,
    )(*args)


def spread_column(rows, length):
    peers = rows.shape[0]
    spread = jnp.broadcast_to(rows, (peers, length, 128)).reshape(peers * length, 128)
    lane = lax.broadcasted_iota(jnp.int32, spread.shape, 1)
    row = lax.rem(lax.broadcasted_iota(jnp.int32, spread.shape, 0), length)
    return jnp.sum(jnp.where(lane == row, spread, 0.0), axis=1, keepdims=True)


def halo_column(halo, turned):
    halo_len, peers = halo.shape
    turned[...] = jnp.zeros_like(turned)
    turned[:halo_len, :peers] = halo[...].astype(F32)
    return spread_column(turned[...].T[:peers].reshape(peers, 1, 128), halo_len)


def fetch(pairs, done):
    return [pltpu.make_async_copy(src, dst, done.at[i]) for i, (src, dst) in enumerate(pairs)]


def first_exchange(
    peers, grp, feat_far, halo_far, request_far, wanted, arrived,
    feat, halo, request, done, turned, asked, outgoing, s0, r0, s1, r1,
):
    links = Links(peers, grp)
    me = links.me
    loads = fetch([(request_far, request), (halo_far, halo), (feat_far, feat)], done)
    for load in loads:
        load.start()
    links.greet()
    nodes = feat.shape[0]
    loads[0].wait()
    loads[1].wait()
    turned[...] = jnp.zeros_like(turned)
    turned[: request.shape[0], :peers] = request[...].astype(F32)
    asked[...] = turned[...].T[:peers].astype(jnp.int32).reshape(asked.shape)
    index = halo_column(halo, turned)
    pick = equal_mask(index, iota((index.shape[0], nodes), 1))
    loads[2].wait()
    outgoing[...] = dot(pick, feat[...]).astype(BF16).reshape(outgoing.shape)
    links.greeted()
    moves = [(block_of(asked), wanted, s0, r0), (block_of(outgoing), arrived, s1, r1)]
    links.start(moves)
    wanted[me] = asked[me]
    arrived[me] = outgoing[me]
    links.finish(moves)


def mark_edges(values, index, marks, nodes, block):
    highs, lows = [], []
    for k, value in enumerate(values):
        node = jnp.where(value < 0, -1, lax.bitwise_and(value, nodes - 1)).astype(F32)
        marks[:, k * 128 : k * 128 + 128] = jnp.where(index[...] == node, 1.0, 0.0).astype(F8)
        source = lax.shift_right_arithmetic(value, nodes.bit_length() - 1)
        highs.append(lax.shift_right_arithmetic(source, block.bit_length() - 1))
        lows.append(lax.bitwise_and(source, block - 1))
    ladder = iota((block, 128), 0).astype(BF16)

    def count(b):
        hits = []
        for high, low in zip(highs, lows):
            here = jnp.where(high == b, low, -1).astype(F32).astype(BF16)
            hits.append(jnp.where(ladder == here, jnp.array(1, BF16), jnp.array(0, BF16)).astype(F8))
        return dot(marks[...], jnp.concatenate(hits, axis=1), NT)

    return count


def count_edges(
    req_len, nodes, block, group, merge, early, src_far, dst_far, count_far, wanted, counts, head,
    src, dst, count, done, total, marks, index, ranks, packs, dense,
):
    loads = fetch([(dst_far, dst), (src_far, src), (count_far, count)], done)
    for load in loads:
        load.start()
    rows, table_rows = counts.shape
    depth = src.shape[0]
    total[...] = jnp.zeros_like(total)
    column = spread_column(wanted[...].astype(F32), req_len)
    index[...] = jnp.broadcast_to(column, index.shape)
    high = jnp.floor(column * (1.0 / 128.0))
    low = column - high * 128.0
    lanes = iota((rows, 128), 1)
    seen = dot(equal_mask(high, lanes), equal_mask(low, lanes), TN)[: nodes // 128]
    power = lax.shift_left(jnp.ones(seen.shape, jnp.int32), lax.broadcasted_iota(jnp.int32, seen.shape, 0))
    word = jnp.sum(jnp.where(seen > 0.5, power, 0), axis=0, keepdims=True)
    lane = lax.broadcasted_iota(jnp.int32, src.shape, 1)
    slot = lax.broadcasted_iota(jnp.int32, src.shape, 0) * 128 + lane
    loads[2].wait()
    live = slot < count[0]
    loads[0].wait()
    into = jnp.where(live, dst[...], 0)
    flags = jnp.take_along_axis(
        jnp.broadcast_to(word, src.shape), lax.bitwise_and(into, 127), axis=1, mode="promise_in_bounds")
    flag = lax.bitwise_and(lax.shift_right_logical(flags, lax.shift_right_logical(into, 7)), 1)
    active = jnp.where(live, flag, 0).astype(F32)
    stride = 128 // merge
    ahead = jnp.where(iota((depth, depth), 1) < iota((depth, depth), 0), 1.0, 0.0).astype(BF16)
    group_sum = active
    before = jnp.zeros_like(active)
    for d in range(1, merge):
        turned = pltpu.roll(active, d * stride, 1)
        group_sum = group_sum + turned
        before = before + jnp.where(lane >= d * stride, turned, 0.0)
    rank = dot(ahead, group_sum.astype(BF16)) + before
    spot = jnp.floor(rank * (1.0 / merge))
    moved = rank - spot * merge - (lane // stride).astype(F32)
    moved = jnp.where(moved < 0.0, moved + merge, moved)
    loads[1].wait()
    pack = src[...] * nodes + into
    for d in range(merge):
        goes = jnp.where((active > 0.5) & (moved == d), spot, -1.0)
        ranks[d] = pltpu.roll(goes, d * stride, 1) if d else goes
        packs[d] = pltpu.roll(pack, d * stride, 1) if d else pack
    most = jnp.max(jnp.sum(group_sum, axis=0, keepdims=True)).astype(jnp.int32)
    longest = (most + merge - 1) // merge
    steps = iota((8, 128), 0)
    for b in range(depth // 8):
        @pl.when((b * 8 < longest) | (b * 8 < early * group))
        def _():
            held = [jnp.full((8, 128), -1, jnp.int32) for _ in range(8)]
            for r in range(8 * b, depth):
                for d in range(merge):
                    to = jnp.broadcast_to(ranks[d, r : r + 1, :], (8, 128))
                    value = jnp.broadcast_to(packs[d, r : r + 1, :], (8, 128))
                    n = (r * merge + d) % len(held)
                    held[n] = jnp.where(to == steps + 8.0 * b, value, held[n])
            while len(held) > 1:
                held = [jnp.maximum(x, y) for x, y in zip(held[::2], held[1::2])]
            dense[8 * b : 8 * b + 8, :] = held[0]
    head[...] = dense[: head.shape[0], :]

    @pl.loop(early, (longest + group - 1) // group)
    def _(c):
        values = [dense[pl.ds(c * group + k, 1), :] for k in range(group)]
        count_block = mark_edges(values, index, marks, nodes, block)
        for b in range(table_rows // block):
            total[:, b * block : b * block + block] += count_block(b)

    counts[...] = total[...].astype(BF16)


def middle(
    dom, grp, req_len, chunk, block, early,
    feat, arrived, counted, head, wanted, halo, w_self, w_neigh, w_hidden, bias, w_out, ends, labels, weight,
    logits, out, g_s, g_n, g_h, g_b, g_o,
    turned, index, feat_w, agg_w, floor, served, received, picks, upper_lower, deltas,
    back_sent, back, hidden_sent, hidden_in, hidden_part, hidden_pieces, hidden_piece, hidden_own, hidden_all,
    small, small_in, small_part, small_parts,
    grad, self_sent, self_in, self_part, self_parts, self_own, self_all,
    neigh_sent, neigh_in, neigh_part, neigh_parts, neigh_own, neigh_all,
    near, far, returned, halo_back, feat_t, agg_t, hidden_t,
    s0, r0, s1, r1, s2, r2, *more,
):
    plane, line = Line("dom", dom), Line("grp", grp)
    in_plane, in_line, all_plane, extra = more[0:8], more[8:18], more[18:24], more[24:]
    links = Links(dom * grp, grp)
    me = links.me
    nodes, width = feat.shape
    rows, table_rows = counted.shape
    size, parts = row_blocks(rows)
    links.greet()
    index[...] = jnp.broadcast_to(spread_column(wanted[...].astype(F32), req_len), index.shape)
    per = size // req_len
    counts = counted
    if early:
        counts, edge_marks = extra
        group = head.shape[0] // early
        for c in range(early):
            have = counts if c else counted
            values = [head[k : k + 1, :] for k in range(c * group, c * group + group)]
            count_block = mark_edges(values, index, edge_marks, nodes, block)
            for b in range(table_rows // block):
                cols = slice(b * block, b * block + block)
                counts[:, cols] = (have[:, cols].astype(F32) + count_block(b)).astype(BF16)
    for i in range(parts):
        span = slice(i * size, i * size + size)
        degree = jnp.sum(counts[span, :].astype(F32), axis=1, keepdims=True)
        floor_deg = jnp.maximum(degree, 1.0)
        total = dot(counts[span, :nodes], feat[...])
        total += dot(counts[span, nodes:], arrived[...].reshape(table_rows - nodes, width))
        agg = (total / floor_deg).astype(BF16)
        own = dot(equal_mask(index[span, :1], iota((size, nodes), 1)), feat[...]).astype(BF16)
        emb = (dot(own, w_self[...]) + dot(agg, w_neigh[...])).astype(BF16)
        served[i * per : i * per + per] = emb.reshape(per, req_len, width)
        feat_w[span, :] = own
        agg_w[span, :] = agg
        floor[span, :] = jnp.broadcast_to(floor_deg, (size, 128))
    links.greeted()
    serve = [(block_of(served), received, s0, r0)]
    links.start(serve)
    received[me] = served[me]
    pairs = ends.shape[1]
    slots = iota((rows, chunk), 0)

    @pl.loop(0, pairs // chunk)
    def _(c):
        span = pl.ds(pl.multiple_of(c * chunk, chunk), chunk)
        end = ends[:, span].astype(F32)
        picks[:rows, span] = equal_mask(slots, end[:1, :])
        picks[rows:, span] = equal_mask(slots, end[1:, :])

    hidden_t[0] = w_hidden[:width, :].T
    hidden_t[1] = w_hidden[width:, :].T
    bias_col = column_of(bias[...])
    out_col = column_of(w_out[...])
    links.finish(serve)

    got = received[...].reshape(rows, width)
    for i, place in enumerate((0, rows)):
        exact = dot(hidden_t[i], got, NT)
        upper = exact.astype(BF16)
        upper_lower[:width, place : place + rows] = upper
        upper_lower[width:, place : place + rows] = (exact - upper.astype(F32)).astype(BF16)

    def step(c, carry):
        bias_sum, out_sum = carry
        span = pl.ds(pl.multiple_of(c * chunk, chunk), chunk)
        both = dot(upper_lower[...], picks[:, span])
        pre = both[:width] + both[width:] + bias_col
        hidden = jnp.maximum(pre, 0.0)
        logit = jnp.sum(hidden * out_col, axis=0, keepdims=True)
        logits[:, span] = logit
        slope = weight[:, span] * (jax.nn.sigmoid(logit) - labels[:, span].astype(F32))
        delta = jnp.where(pre > 0, slope * out_col, 0.0)
        deltas[:, span] = delta.astype(BF16)
        return (
            bias_sum + jnp.sum(delta, axis=1, keepdims=True),
            out_sum + jnp.sum(hidden * slope, axis=1, keepdims=True),
        )

    zero = jnp.zeros((width, 1), F32)
    bias_sum, out_sum = lax.fori_loop(0, pairs // chunk, step, (zero, zero), unroll=True)
    left = dot(picks[:rows, :], deltas[...], NT).astype(BF16)
    right = dot(picks[rows:, :], deltas[...], NT).astype(BF16)
    back_rows = dot(left, w_hidden[:width, :], NT) + dot(right, w_hidden[width:, :], NT)
    back_sent[...] = back_rows.astype(BF16).reshape(back_sent.shape)
    give = [(block_of(back_sent), back, s1, r1)]
    links.start(give)
    back[me] = back_sent[me]

    small[0:1, :] = row_of(bias_sum)
    small[1:2, :] = row_of(out_sum)
    half = dom // 2
    shape = (half,) + hidden_sent.shape[1:]
    hidden_sent[:half] = dot(got, left, TN).astype(BF16).reshape(shape)
    hidden_sent[half:] = dot(got, right, TN).astype(BF16).reshape(shape)
    hidden_first = [(block_of(hidden_sent), hidden_in) + in_plane[0:2], (whole_of(small), small_in) + in_plane[2:4]]
    plane.start(hidden_first)
    hidden_in[plane.me] = hidden_sent[plane.me]
    small_in[plane.me] = small[...]
    other = row_of(index[:, :1])
    halo_row = row_of(halo_column(halo, turned))
    feat_t[...] = feat_w[...].T
    agg_t[...] = agg_w[...].T
    plane.finish(hidden_first)
    hidden_part[...] = jnp.sum(hidden_in[...].astype(F32), axis=0).astype(BF16).reshape(hidden_part.shape)
    small_part[...] = jnp.sum(small_in[...], axis=0)
    hidden_second = [
        (block_of(hidden_part), hidden_pieces) + in_line[0:2],
        (whole_of(small_part), small_parts) + in_line[2:4],
    ]
    line.start(hidden_second)
    hidden_pieces[line.me] = hidden_part[line.me]
    small_parts[line.me] = small_part[...]
    links.finish(give)

    back_all = back[...].reshape(rows, width)
    self_sent[...] = dot(feat_t[...], back_all).astype(BF16).reshape(self_sent.shape)
    self_first = [(block_of(self_sent), self_in) + in_plane[4:6]]
    plane.start(self_first)
    neigh_sent[...] = dot(agg_t[...], back_all).astype(BF16).reshape(neigh_sent.shape)
    neigh_first = [(block_of(neigh_sent), neigh_in) + in_plane[6:8]]
    plane.start(neigh_first)
    for i in range(parts):
        span = slice(i * size, i * size + size)
        same = index[span, :1] == other
        first = lax.broadcasted_iota(jnp.int32, same.shape, 0) + i * size
        earlier = lax.broadcasted_iota(jnp.int32, same.shape, 1) < first
        repeat = jnp.sum(jnp.where(same & earlier, 1.0, 0.0), axis=1, keepdims=True)
        total = dot(jnp.where(same, 1.0, 0.0).astype(BF16), back_all)
        grad[span, :] = jnp.where(repeat > 0.0, 0.0, total).astype(BF16)
    far[...] = (dot(grad[...], w_neigh[...], NT) / floor[:, :1]).astype(BF16)
    returned[...] = dot(counts[:, nodes:], far[...], TN).astype(BF16).reshape(returned.shape)
    send_back = [(block_of(returned), halo_back, s2, r2)]
    links.start(send_back)
    halo_back[me] = returned[me]
    self_in[plane.me] = self_sent[plane.me]
    neigh_in[plane.me] = neigh_sent[plane.me]

    line.finish(hidden_second)
    hidden_piece[...] = jnp.sum(hidden_pieces[...].astype(F32), axis=0).astype(BF16)
    hidden_third = [(whole_of(hidden_piece), hidden_own) + in_line[4:6]]
    line.start(hidden_third)
    hidden_own[line.me] = hidden_piece[...]
    total = jnp.sum(small_parts[...], axis=0)
    g_b[...] = total[0:1, :]
    g_o[...] = total[1:2, :]
    near[...] = dot(grad[...], w_self[...], NT).astype(BF16)

    def local(b, carry):
        cols = pl.ds(pl.multiple_of(b * block, block), block)
        spot = lax.broadcasted_iota(jnp.int32, (1, block), 1) + b * block
        pick = equal_mask(index[:, :1], spot.astype(F32))
        out[cols, :] = dot(counts[:, cols], far[...], TN) + dot(pick, near[...], TN)
        return carry

    cut = nodes // block * 5 // 8
    lax.fori_loop(0, cut, local, 0)
    plane.finish(self_first)
    self_part[...] = jnp.sum(self_in[...].astype(F32), axis=0).astype(BF16)
    self_next = [(whole_of(self_part), self_parts) + in_line[6:8]]
    line.start(self_next)
    self_parts[line.me] = self_part[...]
    lax.fori_loop(cut, nodes // block, local, 0)
    plane.finish(neigh_first)
    neigh_part[...] = jnp.sum(neigh_in[...].astype(F32), axis=0).astype(BF16)
    neigh_next = [(whole_of(neigh_part), neigh_parts) + in_line[8:10]]
    line.start(neigh_next)
    neigh_parts[line.me] = neigh_part[...]

    line.finish(hidden_third)
    hidden_last = [(whole_of(hidden_own), hidden_all) + all_plane[0:2]]
    plane.start(hidden_last)
    hidden_all[plane.me] = hidden_own[...]

    links.finish(send_back)

    def add(b, carry):
        cols = pl.ds(pl.multiple_of(b * block, block), block)
        spot = iota((block, halo_row.shape[1]), 0) + (b * block).astype(F32)
        out[cols, :] += dot(equal_mask(spot, halo_row), halo_back[...].reshape(halo_row.shape[1], width))
        return carry

    lax.fori_loop(0, nodes // block, add, 0)
    line.finish(self_next)
    self_own[...] = jnp.sum(self_parts[...].astype(F32), axis=0).astype(BF16)
    self_last = [(whole_of(self_own), self_all) + all_plane[2:4]]
    plane.start(self_last)
    self_all[plane.me] = self_own[...]
    line.finish(neigh_next)
    neigh_own[...] = jnp.sum(neigh_parts[...].astype(F32), axis=0).astype(BF16)
    neigh_last = [(whole_of(neigh_own), neigh_all) + all_plane[4:6]]
    plane.start(neigh_last)
    neigh_all[plane.me] = neigh_own[...]
    plane.finish(hidden_last)
    g_h[...] = hidden_all[...].astype(F32).reshape(g_h.shape)
    plane.finish(self_last)
    g_s[...] = self_all[...].astype(F32).reshape(g_s.shape)
    plane.finish(neigh_last)
    g_n[...] = neigh_all[...].astype(F32).reshape(g_n.shape)


def put_out(count, *refs):
    sent, kept, done = refs[:count], refs[count : 2 * count], refs[2 * count]
    copies = [pltpu.make_async_copy(src, dst, done.at[i]) for i, (src, dst) in enumerate(zip(sent, kept))]
    for copy in copies:
        copy.start()
    for copy in copies:
        copy.wait()


def store(values):
    count = len(values)
    return pl.pallas_call(
        functools.partial(put_out, count),
        out_shape=tuple(jax.ShapeDtypeStruct(v.shape, v.dtype) for v in values),
        in_specs=[pl.BlockSpec(memory_space=pltpu.VMEM)] * count,
        out_specs=tuple(pl.BlockSpec(memory_space=pl.ANY) for _ in values),
        scratch_shapes=[pltpu.SemaphoreType.DMA((count,))],
        compiler_params=pltpu.CompilerParams(vmem_limit_bytes=8 * 1024 * 1024),
    )(*values)


def row_blocks(rows):
    size = min(rows, 512)
    return size, rows // size


def per_device(
    features, edge_src, edge_dst, edge_count, halo_index, request_rows, pair_ends,
    labels, pair_weight, w_self, w_neigh, w_hidden, b_hidden, w_out,
):
    nodes, width = features.shape
    grp = lax.axis_size("grp")
    dom = lax.axis_size("dom")
    peers = dom * grp
    halo_len = halo_index.shape[2]
    req_len = request_rows.shape[2]
    slots = edge_src.shape[0]
    pairs = labels.shape[0]
    table_rows = nodes + peers * halo_len
    rows = peers * req_len
    block = 256
    piece = width // dom
    turn = max(128, peers)

    halo = halo_index[0].T
    wanted, arrived = call(
        functools.partial(first_exchange, peers, grp),
        [((peers, 1, 128), jnp.int32), ((peers, halo_len, width), BF16)],
        (features, halo, request_rows[0].T),
        [
            pltpu.VMEM((nodes, width), BF16),
            pltpu.VMEM((halo_len, peers), jnp.int32),
            pltpu.VMEM((req_len, peers), jnp.int32),
            pltpu.SemaphoreType.DMA((3,)),
            pltpu.VMEM((128, turn), F32),
            pltpu.VMEM((peers, 1, 128), jnp.int32),
            pltpu.VMEM((peers, halo_len, width), BF16),
        ] + sems(peers, 2),
        collective_id=0,
        hbm=(0, 1, 2),
        limit=K1LIM,
        micros=10,
    )
    group = 8
    depth = slots // 128
    merge = 2
    early = 3 if rows <= 1024 else 0
    counts, head = call(
        functools.partial(count_edges, req_len, nodes, block, group, merge, early),
        [((rows, table_rows), BF16), ((max(early, 1) * group, 128), jnp.int32)],
        (edge_src.reshape(depth, 128), edge_dst.reshape(depth, 128), edge_count, wanted),
        [
            pltpu.VMEM((depth, 128), jnp.int32),
            pltpu.VMEM((depth, 128), jnp.int32),
            pltpu.SMEM((1,), jnp.int32),
            pltpu.SemaphoreType.DMA((3,)),
            pltpu.VMEM((rows, table_rows), F32),
            pltpu.VMEM((rows, group * 128), F8),
            pltpu.VMEM((rows, 128), F32),
            pltpu.VMEM((merge, depth, 128), F32),
            pltpu.VMEM((merge, depth, 128), jnp.int32),
            pltpu.VMEM((depth, 128), jnp.int32),
        ],
        hbm=(0, 1, 2),
        micros=10,
        limit=min(VMEM_LIMIT, rows * 40 * 1024),
    )
    chunk = 256
    rows_of = lambda *shape: pltpu.VMEM(shape, BF16)
    found = call(
        functools.partial(middle, dom, grp, req_len, chunk, block, early),
        [
            ((1, pairs), F32),
            ((nodes, width), F32),
            ((width, width), F32),
            ((width, width), F32),
            ((2 * width, width), F32),
            ((1, width), F32),
            ((1, width), F32),
        ],
        (
            features, arrived, counts, head, wanted, halo, w_self, w_neigh, w_hidden,
            b_hidden.reshape(1, width), w_out.reshape(1, width),
            pair_ends.T, labels.reshape(1, pairs), pair_weight.reshape(1, pairs),
        ),
        [
            pltpu.VMEM((128, turn), F32),
            pltpu.VMEM((rows, 128), F32),
            rows_of(rows, width),
            rows_of(rows, width),
            pltpu.VMEM((rows, 128), F32),
            rows_of(peers, req_len, width),
            rows_of(peers, req_len, width),
            rows_of(2 * rows, pairs),
            rows_of(2 * width, 2 * rows),
            rows_of(width, pairs),
            rows_of(peers, req_len, width),
            rows_of(peers, req_len, width),
            rows_of(dom, 2 * piece, width),
            rows_of(dom, 2 * piece, width),
            rows_of(grp, 2 * piece // grp, width),
            rows_of(grp, 2 * piece // grp, width),
            rows_of(2 * piece // grp, width),
            rows_of(grp, 2 * piece // grp, width),
            rows_of(dom, grp, 2 * piece // grp, width),
            pltpu.VMEM((2, width), F32),
            pltpu.VMEM((dom, 2, width), F32),
            pltpu.VMEM((2, width), F32),
            pltpu.VMEM((grp, 2, width), F32),
            rows_of(rows, width),
        ] + 2 * [
            rows_of(dom, piece, width),
            rows_of(dom, piece, width),
            rows_of(piece, width),
            rows_of(grp, piece, width),
            rows_of(piece, width),
            rows_of(dom, piece, width),
        ] + [
            rows_of(rows, width),
            rows_of(rows, width),
            rows_of(peers, halo_len, width),
            rows_of(peers, halo_len, width),
            rows_of(width, rows),
            rows_of(width, rows),
            rows_of(2, width, width),
        ] + sems(peers, 3) + sems(dom, 4) + sems(grp, 5) + sems(dom, 3) + min(early, 1) * [rows_of(rows, table_rows), pltpu.VMEM((rows, group * 128), F8)],
        collective_id=1,
        limit=min(VMEM_LIMIT, rows * 60 * 1024),
    )
    logits, grad_features, g_s, g_n, g_h, g_b, g_o = store(found)
    return (logits.reshape(pairs), grad_features, g_s, g_n, g_h, g_b.reshape(width), g_o.reshape(width))


def solution(mesh):
    both = ("dom", "grp")
    in_specs = (
        P(both, None), P(both), P(both), P(both), P(both, None, None), P(both, None, None),
        P(both, None), P(both), P(both), P(), P(), P(), P(), P(),
    )
    out_specs = (P(both), P(both, None), P(), P(), P(), P(), P())
    return jax.shard_map(
        per_device, mesh=mesh, in_specs=in_specs, out_specs=out_specs, check_vma=False
    )
```

```python
import functools

import jax
import jax.numpy as jnp
from jax import lax
from jax.experimental import pallas as pl
from jax.experimental.pallas import tpu as pltpu
from jax.sharding import PartitionSpec as P

F32 = jnp.float32
BF16 = jnp.bfloat16
F8 = jnp.float8_e4m3fn
VMEM_LIMIT = 63 * 1024 * 1024
K1LIM = 64 * 1024 * 1024 - 512 * 1024
NN = (((1,), (0,)), ((), ()))
NT = (((1,), (1,)), ((), ()))
TN = (((0,), (0,)), ((), ()))


def dot(left, right, dims=NN):
    return lax.dot_general(left, right, dims, preferred_element_type=F32)


def column_of(row):
    return jnp.broadcast_to(row, (128, row.shape[1])).T[:, :1]


def row_of(column):
    return jnp.broadcast_to(column, (column.shape[0], 128)).T[:1, :]


def equal_mask(left, right):
    return jnp.where(left == right, 1.0, 0.0).astype(BF16)


def iota(shape, dim):
    return lax.broadcasted_iota(jnp.int32, shape, dim).astype(F32)


class Links:
    def __init__(self, peers, grp):
        self.peers, self.grp = peers, grp
        self.me = lax.axis_index("dom") * grp + lax.axis_index("grp")

    def device(self, peer):
        return {"dom": peer // self.grp, "grp": lax.rem(peer, self.grp)}

    def other(self, step):
        return lax.rem(self.me + step, self.peers)

    def each(self, body):
        def step(i, carry):
            body(self.other(i))
            return carry

        lax.fori_loop(1, self.peers, step, 0, unroll=self.peers - 1 if self.peers <= 32 else 1)

    def greet(self):
        barrier = pltpu.get_barrier_semaphore()
        self.each(lambda peer: pl.semaphore_signal(
            barrier, inc=1, device_id=self.device(peer), device_id_type=pl.DeviceIdType.MESH))

    def greeted(self):
        pl.semaphore_wait(pltpu.get_barrier_semaphore(), self.peers - 1)

    def copy(self, src, dst, send, recv, peer, slot):
        return pltpu.make_async_remote_copy(
            src_ref=src, dst_ref=dst, send_sem=send.at[peer], recv_sem=recv.at[slot],
            device_id=self.device(peer), device_id_type=pl.DeviceIdType.MESH)

    def start(self, moves):
        def one(peer):
            for pick, dst, send, recv in moves:
                self.copy(pick(peer), dst.at[self.me], send, recv, peer, self.me).start()

        self.each(one)

    def finish(self, moves):
        def one(peer):
            for pick, dst, send, recv in moves:
                copy = self.copy(pick(peer), dst.at[peer], send, recv, peer, peer)
                copy.wait_recv()
                copy.wait_send()

        self.each(one)


class Line(Links):
    def __init__(self, axis, peers):
        self.axis, self.peers = axis, peers
        self.me = lax.axis_index(axis)

    def device(self, peer):
        return {self.axis: peer}


def block_of(ref):
    return lambda peer: ref.at[peer]


def whole_of(ref):
    return lambda peer: ref


def sems(peers, count):
    return [pltpu.SemaphoreType.DMA((peers,)) for _ in range(2 * count)]


def call(body, outs, args, scratch=(), collective_id=None, hbm=(), limit=VMEM_LIMIT, micros=0):
    params = dict(vmem_limit_bytes=limit)
    if collective_id is not None:
        params.update(collective_id=collective_id, has_side_effects=True)
    return pl.pallas_call(
        body,
        out_shape=tuple(jax.ShapeDtypeStruct(s, d) for s, d in outs),
        in_specs=[
            pl.BlockSpec(memory_space=pltpu.HBM if i in hbm else pltpu.VMEM)
            for i in range(len(args))
        ],
        out_specs=tuple(pl.BlockSpec(memory_space=pltpu.VMEM) for _ in outs),
        scratch_shapes=list(scratch),
        compiler_params=pltpu.CompilerParams(**params),
        cost_estimate=pl.CostEstimate(flops=micros * 10**9, bytes_accessed=1024, transcendentals=0) if micros else None,
    )(*args)


def spread_column(rows, length):
    peers = rows.shape[0]
    spread = jnp.broadcast_to(rows, (peers, length, 128)).reshape(peers * length, 128)
    lane = lax.broadcasted_iota(jnp.int32, spread.shape, 1)
    row = lax.rem(lax.broadcasted_iota(jnp.int32, spread.shape, 0), length)
    return jnp.sum(jnp.where(lane == row, spread, 0.0), axis=1, keepdims=True)


def halo_column(halo, turned):
    halo_len, peers = halo.shape
    turned[...] = jnp.zeros_like(turned)
    turned[:halo_len, :peers] = halo[...].astype(F32)
    return spread_column(turned[...].T[:peers].reshape(peers, 1, 128), halo_len)


def fetch(pairs, done):
    return [pltpu.make_async_copy(src, dst, done.at[i]) for i, (src, dst) in enumerate(pairs)]


def first_exchange(
    peers, grp, feat_far, halo_far, request_far, wanted, arrived,
    feat, halo, request, done, turned, asked, outgoing, s0, r0, s1, r1,
):
    links = Links(peers, grp)
    me = links.me
    loads = fetch([(request_far, request), (halo_far, halo), (feat_far, feat)], done)
    for load in loads:
        load.start()
    links.greet()
    nodes = feat.shape[0]
    loads[0].wait()
    loads[1].wait()
    turned[...] = jnp.zeros_like(turned)
    turned[: request.shape[0], :peers] = request[...].astype(F32)
    asked[...] = turned[...].T[:peers].astype(jnp.int32).reshape(asked.shape)
    index = halo_column(halo, turned)
    pick = equal_mask(index, iota((index.shape[0], nodes), 1))
    loads[2].wait()
    outgoing[...] = dot(pick, feat[...]).astype(BF16).reshape(outgoing.shape)
    links.greeted()
    moves = [(block_of(asked), wanted, s0, r0), (block_of(outgoing), arrived, s1, r1)]
    links.start(moves)
    wanted[me] = asked[me]
    arrived[me] = outgoing[me]
    links.finish(moves)


def mark_edges(values, index, marks, nodes, block):
    highs, lows = [], []
    for k, value in enumerate(values):
        node = jnp.where(value < 0, -1, lax.bitwise_and(value, nodes - 1)).astype(F32)
        marks[:, k * 128 : k * 128 + 128] = jnp.where(index[...] == node, 1.0, 0.0).astype(F8)
        source = lax.shift_right_arithmetic(value, nodes.bit_length() - 1)
        highs.append(lax.shift_right_arithmetic(source, block.bit_length() - 1))
        lows.append(lax.bitwise_and(source, block - 1))
    ladder = iota((block, 128), 0).astype(BF16)

    def count(b):
        hits = []
        for high, low in zip(highs, lows):
            here = jnp.where(high == b, low, -1).astype(F32).astype(BF16)
            hits.append(jnp.where(ladder == here, jnp.array(1, BF16), jnp.array(0, BF16)).astype(F8))
        return dot(marks[...], jnp.concatenate(hits, axis=1), NT)

    return count


def count_edges(
    req_len, nodes, block, group, merge, early, src_far, dst_far, count_far, wanted, counts, head,
    src, dst, count, done, total, marks, index, ranks, packs, dense,
):
    loads = fetch([(dst_far, dst), (src_far, src), (count_far, count)], done)
    for load in loads:
        load.start()
    rows, table_rows = counts.shape
    depth = src.shape[0]
    total[...] = jnp.zeros_like(total)
    column = spread_column(wanted[...].astype(F32), req_len)
    index[...] = jnp.broadcast_to(column, index.shape)
    high = jnp.floor(column * (1.0 / 128.0))
    low = column - high * 128.0
    lanes = iota((rows, 128), 1)
    seen = dot(equal_mask(high, lanes), equal_mask(low, lanes), TN)[: nodes // 128]
    power = lax.shift_left(jnp.ones(seen.shape, jnp.int32), lax.broadcasted_iota(jnp.int32, seen.shape, 0))
    word = jnp.sum(jnp.where(seen > 0.5, power, 0), axis=0, keepdims=True)
    lane = lax.broadcasted_iota(jnp.int32, src.shape, 1)
    slot = lax.broadcasted_iota(jnp.int32, src.shape, 0) * 128 + lane
    loads[2].wait()
    live = slot < count[0]
    loads[0].wait()
    into = jnp.where(live, dst[...], 0)
    flags = jnp.take_along_axis(
        jnp.broadcast_to(word, src.shape), lax.bitwise_and(into, 127), axis=1, mode="promise_in_bounds")
    flag = lax.bitwise_and(lax.shift_right_logical(flags, lax.shift_right_logical(into, 7)), 1)
    active = jnp.where(live, flag, 0).astype(F32)
    stride = 128 // merge
    ahead = jnp.where(iota((depth, depth), 1) < iota((depth, depth), 0), 1.0, 0.0).astype(BF16)
    group_sum = active
    before = jnp.zeros_like(active)
    for d in range(1, merge):
        turned = pltpu.roll(active, d * stride, 1)
        group_sum = group_sum + turned
        before = before + jnp.where(lane >= d * stride, turned, 0.0)
    rank = dot(ahead, group_sum.astype(BF16)) + before
    spot = jnp.floor(rank * (1.0 / merge))
    moved = rank - spot * merge - (lane // stride).astype(F32)
    moved = jnp.where(moved < 0.0, moved + merge, moved)
    loads[1].wait()
    pack = src[...] * nodes + into
    for d in range(merge):
        goes = jnp.where((active > 0.5) & (moved == d), spot, -1.0)
        ranks[d] = pltpu.roll(goes, d * stride, 1) if d else goes
        packs[d] = pltpu.roll(pack, d * stride, 1) if d else pack
    most = jnp.max(jnp.sum(group_sum, axis=0, keepdims=True)).astype(jnp.int32)
    longest = (most + merge - 1) // merge
    steps = iota((8, 128), 0)
    for b in range(depth // 8):
        @pl.when((b * 8 < longest) | (b * 8 < early * group))
        def _():
            held = [jnp.full((8, 128), -1, jnp.int32) for _ in range(8)]
            for r in range(8 * b, depth):
                for d in range(merge):
                    to = jnp.broadcast_to(ranks[d, r : r + 1, :], (8, 128))
                    value = jnp.broadcast_to(packs[d, r : r + 1, :], (8, 128))
                    n = (r * merge + d) % len(held)
                    held[n] = jnp.where(to == steps + 8.0 * b, value, held[n])
            while len(held) > 1:
                held = [jnp.maximum(x, y) for x, y in zip(held[::2], held[1::2])]
            dense[8 * b : 8 * b + 8, :] = held[0]
    head[...] = dense[: head.shape[0], :]

    @pl.loop(early, (longest + group - 1) // group)
    def _(c):
        values = [dense[pl.ds(c * group + k, 1), :] for k in range(group)]
        count_block = mark_edges(values, index, marks, nodes, block)
        for b in range(table_rows // block):
            total[:, b * block : b * block + block] += count_block(b)

    counts[...] = total[...].astype(BF16)


def middle(
    dom, grp, req_len, chunk, block, early,
    feat, arrived, counted, head, wanted, halo, w_self, w_neigh, w_hidden, bias, w_out, ends, labels, weight,
    logits, out, g_s, g_n, g_h, g_b, g_o,
    turned, index, feat_w, agg_w, floor, served, received, picks, upper_lower, deltas,
    back_sent, back, hidden_sent, hidden_in, hidden_part, hidden_pieces, hidden_piece, hidden_own, hidden_all,
    small, small_in, small_part, small_parts,
    grad, self_sent, self_in, self_part, self_parts, self_own, self_all,
    neigh_sent, neigh_in, neigh_part, neigh_parts, neigh_own, neigh_all,
    near, far, returned, halo_back, feat_t, agg_t, hidden_t,
    s0, r0, s1, r1, s2, r2, *more,
):
    plane, line = Line("dom", dom), Line("grp", grp)
    in_plane, in_line, all_plane, extra = more[0:8], more[8:18], more[18:24], more[24:]
    links = Links(dom * grp, grp)
    me = links.me
    nodes, width = feat.shape
    rows, table_rows = counted.shape
    size, parts = row_blocks(rows)
    links.greet()
    index[...] = jnp.broadcast_to(spread_column(wanted[...].astype(F32), req_len), index.shape)
    per = size // req_len
    counts = counted
    if early:
        counts, edge_marks = extra
        group = head.shape[0] // early
        for c in range(early):
            have = counts if c else counted
            values = [head[k : k + 1, :] for k in range(c * group, c * group + group)]
            count_block = mark_edges(values, index, edge_marks, nodes, block)
            for b in range(table_rows // block):
                cols = slice(b * block, b * block + block)
                counts[:, cols] = (have[:, cols].astype(F32) + count_block(b)).astype(BF16)
    for i in range(parts):
        span = slice(i * size, i * size + size)
        degree = jnp.sum(counts[span, :].astype(F32), axis=1, keepdims=True)
        floor_deg = jnp.maximum(degree, 1.0)
        total = dot(counts[span, :nodes], feat[...])
        total += dot(counts[span, nodes:], arrived[...].reshape(table_rows - nodes, width))
        agg = (total / floor_deg).astype(BF16)
        own = dot(equal_mask(index[span, :1], iota((size, nodes), 1)), feat[...]).astype(BF16)
        emb = (dot(own, w_self[...]) + dot(agg, w_neigh[...])).astype(BF16)
        served[i * per : i * per + per] = emb.reshape(per, req_len, width)
        feat_w[span, :] = own
        agg_w[span, :] = agg
        floor[span, :] = jnp.broadcast_to(floor_deg, (size, 128))
    links.greeted()
    serve = [(block_of(served), received, s0, r0)]
    links.start(serve)
    received[me] = served[me]
    pairs = ends.shape[1]
    slots = iota((rows, chunk), 0)

    @pl.loop(0, pairs // chunk)
    def _(c):
        span = pl.ds(pl.multiple_of(c * chunk, chunk), chunk)
        end = ends[:, span].astype(F32)
        picks[:rows, span] = equal_mask(slots, end[:1, :])
        picks[rows:, span] = equal_mask(slots, end[1:, :])

    hidden_t[0] = w_hidden[:width, :].T
    hidden_t[1] = w_hidden[width:, :].T
    bias_col = column_of(bias[...])
    out_col = column_of(w_out[...])
    links.finish(serve)

    got = received[...].reshape(rows, width)
    for i, place in enumerate((0, rows)):
        exact = dot(hidden_t[i], got, NT)
        upper = exact.astype(BF16)
        upper_lower[:width, place : place + rows] = upper
        upper_lower[width:, place : place + rows] = (exact - upper.astype(F32)).astype(BF16)

    def step(c, carry):
        bias_sum, out_sum = carry
        span = pl.ds(pl.multiple_of(c * chunk, chunk), chunk)
        both = dot(upper_lower[...], picks[:, span])
        pre = both[:width] + both[width:] + bias_col
        hidden = jnp.maximum(pre, 0.0)
        logit = jnp.sum(hidden * out_col, axis=0, keepdims=True)
        logits[:, span] = logit
        slope = weight[:, span] * (jax.nn.sigmoid(logit) - labels[:, span].astype(F32))
        delta = jnp.where(pre > 0, slope * out_col, 0.0)
        deltas[:, span] = delta.astype(BF16)
        return (
            bias_sum + jnp.sum(delta, axis=1, keepdims=True),
            out_sum + jnp.sum(hidden * slope, axis=1, keepdims=True),
        )

    zero = jnp.zeros((width, 1), F32)
    bias_sum, out_sum = lax.fori_loop(0, pairs // chunk, step, (zero, zero), unroll=True)
    left = dot(picks[:rows, :], deltas[...], NT).astype(BF16)
    right = dot(picks[rows:, :], deltas[...], NT).astype(BF16)
    back_rows = dot(left, w_hidden[:width, :], NT) + dot(right, w_hidden[width:, :], NT)
    back_sent[...] = back_rows.astype(BF16).reshape(back_sent.shape)
    give = [(block_of(back_sent), back, s1, r1)]
    links.start(give)
    back[me] = back_sent[me]

    small[0:1, :] = row_of(bias_sum)
    small[1:2, :] = row_of(out_sum)
    half = dom // 2
    shape = (half,) + hidden_sent.shape[1:]
    hidden_sent[:half] = dot(got, left, TN).astype(BF16).reshape(shape)
    hidden_sent[half:] = dot(got, right, TN).astype(BF16).reshape(shape)
    hidden_first = [(block_of(hidden_sent), hidden_in) + in_plane[0:2], (whole_of(small), small_in) + in_plane[2:4]]
    plane.start(hidden_first)
    hidden_in[plane.me] = hidden_sent[plane.me]
    small_in[plane.me] = small[...]
    other = row_of(index[:, :1])
    halo_row = row_of(halo_column(halo, turned))
    feat_t[...] = feat_w[...].T
    agg_t[...] = agg_w[...].T
    plane.finish(hidden_first)
    hidden_part[...] = jnp.sum(hidden_in[...].astype(F32), axis=0).astype(BF16).reshape(hidden_part.shape)
    small_part[...] = jnp.sum(small_in[...], axis=0)
    hidden_second = [
        (block_of(hidden_part), hidden_pieces) + in_line[0:2],
        (whole_of(small_part), small_parts) + in_line[2:4],
    ]
    line.start(hidden_second)
    hidden_pieces[line.me] = hidden_part[line.me]
    small_parts[line.me] = small_part[...]
    links.finish(give)

    back_all = back[...].reshape(rows, width)
    self_sent[...] = dot(feat_t[...], back_all).astype(BF16).reshape(self_sent.shape)
    self_first = [(block_of(self_sent), self_in) + in_plane[4:6]]
    plane.start(self_first)
    neigh_sent[...] = dot(agg_t[...], back_all).astype(BF16).reshape(neigh_sent.shape)
    neigh_first = [(block_of(neigh_sent), neigh_in) + in_plane[6:8]]
    plane.start(neigh_first)
    for i in range(parts):
        span = slice(i * size, i * size + size)
        same = index[span, :1] == other
        first = lax.broadcasted_iota(jnp.int32, same.shape, 0) + i * size
        earlier = lax.broadcasted_iota(jnp.int32, same.shape, 1) < first
        repeat = jnp.sum(jnp.where(same & earlier, 1.0, 0.0), axis=1, keepdims=True)
        total = dot(jnp.where(same, 1.0, 0.0).astype(BF16), back_all)
        grad[span, :] = jnp.where(repeat > 0.0, 0.0, total).astype(BF16)
    far[...] = (dot(grad[...], w_neigh[...], NT) / floor[:, :1]).astype(BF16)
    returned[...] = dot(counts[:, nodes:], far[...], TN).astype(BF16).reshape(returned.shape)
    send_back = [(block_of(returned), halo_back, s2, r2)]
    links.start(send_back)
    halo_back[me] = returned[me]
    self_in[plane.me] = self_sent[plane.me]
    neigh_in[plane.me] = neigh_sent[plane.me]

    line.finish(hidden_second)
    hidden_piece[...] = jnp.sum(hidden_pieces[...].astype(F32), axis=0).astype(BF16)
    hidden_third = [(whole_of(hidden_piece), hidden_own) + in_line[4:6]]
    line.start(hidden_third)
    hidden_own[line.me] = hidden_piece[...]
    total = jnp.sum(small_parts[...], axis=0)
    g_b[...] = total[0:1, :]
    g_o[...] = total[1:2, :]
    near[...] = dot(grad[...], w_self[...], NT).astype(BF16)

    def local(b, carry):
        cols = pl.ds(pl.multiple_of(b * block, block), block)
        spot = lax.broadcasted_iota(jnp.int32, (1, block), 1) + b * block
        pick = equal_mask(index[:, :1], spot.astype(F32))
        out[cols, :] = dot(counts[:, cols], far[...], TN) + dot(pick, near[...], TN)
        return carry

    cut = nodes // block * 5 // 8
    lax.fori_loop(0, cut, local, 0)
    plane.finish(self_first)
    self_part[...] = jnp.sum(self_in[...].astype(F32), axis=0).astype(BF16)
    self_next = [(whole_of(self_part), self_parts) + in_line[6:8]]
    line.start(self_next)
    self_parts[line.me] = self_part[...]
    lax.fori_loop(cut, nodes // block, local, 0)
    plane.finish(neigh_first)
    neigh_part[...] = jnp.sum(neigh_in[...].astype(F32), axis=0).astype(BF16)
    neigh_next = [(whole_of(neigh_part), neigh_parts) + in_line[8:10]]
    line.start(neigh_next)
    neigh_parts[line.me] = neigh_part[...]

    line.finish(hidden_third)
    hidden_last = [(whole_of(hidden_own), hidden_all) + all_plane[0:2]]
    plane.start(hidden_last)
    hidden_all[plane.me] = hidden_own[...]

    links.finish(send_back)

    def add(b, carry):
        cols = pl.ds(pl.multiple_of(b * block, block), block)
        spot = iota((block, halo_row.shape[1]), 0) + (b * block).astype(F32)
        out[cols, :] += dot(equal_mask(spot, halo_row), halo_back[...].reshape(halo_row.shape[1], width))
        return carry

    lax.fori_loop(0, nodes // block, add, 0)
    line.finish(self_next)
    self_own[...] = jnp.sum(self_parts[...].astype(F32), axis=0).astype(BF16)
    self_last = [(whole_of(self_own), self_all) + all_plane[2:4]]
    plane.start(self_last)
    self_all[plane.me] = self_own[...]
    line.finish(neigh_next)
    neigh_own[...] = jnp.sum(neigh_parts[...].astype(F32), axis=0).astype(BF16)
    neigh_last = [(whole_of(neigh_own), neigh_all) + all_plane[4:6]]
    plane.start(neigh_last)
    neigh_all[plane.me] = neigh_own[...]
    plane.finish(hidden_last)
    g_h[...] = hidden_all[...].astype(F32).reshape(g_h.shape)
    plane.finish(self_last)
    g_s[...] = self_all[...].astype(F32).reshape(g_s.shape)
    plane.finish(neigh_last)
    g_n[...] = neigh_all[...].astype(F32).reshape(g_n.shape)


def put_out(count, *refs):
    sent, kept, done = refs[:count], refs[count : 2 * count], refs[2 * count]
    copies = [pltpu.make_async_copy(src, dst, done.at[i]) for i, (src, dst) in enumerate(zip(sent, kept))]
    for copy in copies:
        copy.start()
    for copy in copies:
        copy.wait()


def store(values):
    count = len(values)
    return pl.pallas_call(
        functools.partial(put_out, count),
        out_shape=tuple(jax.ShapeDtypeStruct(v.shape, v.dtype) for v in values),
        in_specs=[pl.BlockSpec(memory_space=pltpu.VMEM)] * count,
        out_specs=tuple(pl.BlockSpec(memory_space=pl.ANY) for _ in values),
        scratch_shapes=[pltpu.SemaphoreType.DMA((count,))],
        compiler_params=pltpu.CompilerParams(vmem_limit_bytes=8 * 1024 * 1024),
    )(*values)


def row_blocks(rows):
    size = min(rows, 512)
    return size, rows // size


def per_device(
    features, edge_src, edge_dst, edge_count, halo_index, request_rows, pair_ends,
    labels, pair_weight, w_self, w_neigh, w_hidden, b_hidden, w_out,
):
    nodes, width = features.shape
    grp = lax.axis_size("grp")
    dom = lax.axis_size("dom")
    peers = dom * grp
    halo_len = halo_index.shape[2]
    req_len = request_rows.shape[2]
    slots = edge_src.shape[0]
    pairs = labels.shape[0]
    table_rows = nodes + peers * halo_len
    rows = peers * req_len
    block = 256
    piece = width // dom
    turn = max(128, peers)

    halo = halo_index[0].T
    wanted, arrived = call(
        functools.partial(first_exchange, peers, grp),
        [((peers, 1, 128), jnp.int32), ((peers, halo_len, width), BF16)],
        (features, halo, request_rows[0].T),
        [
            pltpu.VMEM((nodes, width), BF16),
            pltpu.VMEM((halo_len, peers), jnp.int32),
            pltpu.VMEM((req_len, peers), jnp.int32),
            pltpu.SemaphoreType.DMA((3,)),
            pltpu.VMEM((128, turn), F32),
            pltpu.VMEM((peers, 1, 128), jnp.int32),
            pltpu.VMEM((peers, halo_len, width), BF16),
        ] + sems(peers, 2),
        collective_id=0,
        hbm=(0, 1, 2),
        limit=K1LIM,
        micros=10,
    )
    group = 8
    depth = slots // 128
    merge = 2
    early = 3 if rows <= 1024 else 0
    counts, head = call(
        functools.partial(count_edges, req_len, nodes, block, group, merge, early),
        [((rows, table_rows), BF16), ((max(early, 1) * group, 128), jnp.int32)],
        (edge_src.reshape(depth, 128), edge_dst.reshape(depth, 128), edge_count, wanted),
        [
            pltpu.VMEM((depth, 128), jnp.int32),
            pltpu.VMEM((depth, 128), jnp.int32),
            pltpu.SMEM((1,), jnp.int32),
            pltpu.SemaphoreType.DMA((3,)),
            pltpu.VMEM((rows, table_rows), F32),
            pltpu.VMEM((rows, group * 128), F8),
            pltpu.VMEM((rows, 128), F32),
            pltpu.VMEM((merge, depth, 128), F32),
            pltpu.VMEM((merge, depth, 128), jnp.int32),
            pltpu.VMEM((depth, 128), jnp.int32),
        ],
        hbm=(0, 1, 2),
        micros=10,
        limit=min(VMEM_LIMIT, rows * 40 * 1024),
    )
    chunk = 256
    rows_of = lambda *shape: pltpu.VMEM(shape, BF16)
    found = call(
        functools.partial(middle, dom, grp, req_len, chunk, block, early),
        [
            ((1, pairs), F32),
            ((nodes, width), F32),
            ((width, width), F32),
            ((width, width), F32),
            ((2 * width, width), F32),
            ((1, width), F32),
            ((1, width), F32),
        ],
        (
            features, arrived, counts, head, wanted, halo, w_self, w_neigh, w_hidden,
            b_hidden.reshape(1, width), w_out.reshape(1, width),
            pair_ends.T, labels.reshape(1, pairs), pair_weight.reshape(1, pairs),
        ),
        [
            pltpu.VMEM((128, turn), F32),
            pltpu.VMEM((rows, 128), F32),
            rows_of(rows, width),
            rows_of(rows, width),
            pltpu.VMEM((rows, 128), F32),
            rows_of(peers, req_len, width),
            rows_of(peers, req_len, width),
            rows_of(2 * rows, pairs),
            rows_of(2 * width, 2 * rows),
            rows_of(width, pairs),
            rows_of(peers, req_len, width),
            rows_of(peers, req_len, width),
            rows_of(dom, 2 * piece, width),
            rows_of(dom, 2 * piece, width),
            rows_of(grp, 2 * piece // grp, width),
            rows_of(grp, 2 * piece // grp, width),
            rows_of(2 * piece // grp, width),
            rows_of(grp, 2 * piece // grp, width),
            rows_of(dom, grp, 2 * piece // grp, width),
            pltpu.VMEM((2, width), F32),
            pltpu.VMEM((dom, 2, width), F32),
            pltpu.VMEM((2, width), F32),
            pltpu.VMEM((grp, 2, width), F32),
            rows_of(rows, width),
        ] + 2 * [
            rows_of(dom, piece, width),
            rows_of(dom, piece, width),
            rows_of(piece, width),
            rows_of(grp, piece, width),
            rows_of(piece, width),
            rows_of(dom, piece, width),
        ] + [
            rows_of(rows, width),
            rows_of(rows, width),
            rows_of(peers, halo_len, width),
            rows_of(peers, halo_len, width),
            rows_of(width, rows),
            rows_of(width, rows),
            rows_of(2, width, width),
        ] + sems(peers, 3) + sems(dom, 4) + sems(grp, 5) + sems(dom, 3) + min(early, 1) * [rows_of(rows, table_rows), pltpu.VMEM((rows, group * 128), F8)],
        collective_id=1,
        limit=min(VMEM_LIMIT, rows * 60 * 1024),
    )
    logits, grad_features, g_s, g_n, g_h, g_b, g_o = store(found)
    return (logits.reshape(pairs), grad_features, g_s, g_n, g_h, g_b.reshape(width), g_o.reshape(width))


def solution(mesh):
    both = ("dom", "grp")
    in_specs = (
        P(both, None), P(both), P(both), P(both), P(both, None, None), P(both, None, None),
        P(both, None), P(both), P(both), P(), P(), P(), P(), P(),
    )
    out_specs = (P(both), P(both, None), P(), P(), P(), P(), P())
    return jax.shard_map(
        per_device, mesh=mesh, in_specs=in_specs, out_specs=out_specs, check_vma=False
    )
```
